32 devices in a mesh: sec: 2 (over y), ty: 16 (over z, x, core).
Axes of the slice: x: 2, y: 2, z: 4, core: 2. Of those that a mesh axis runs over, the one named last changes fastest.
Arguments:
- points: float32 [4, 32768], P(None, ('sec', 'ty')), parts along dimension 1, may hold values from -88 to 2136, as said below
- source: bfloat16 [1024, 2048], P(('sec', 'ty')), parts along dimension 0, may hold values from -4 to 4
- slab_first: int32 [32], P(('sec', 'ty')), parts along dimension 0, may hold values from 0 to 29, as said below
- slab_count: int32 [32], P(('sec', 'ty')), parts along dimension 0, may hold values from 3 to 6, as said below
Outputs:
- rendered: bfloat16 [1024, 2048], P(('sec', 'ty')), parts along dimension 0
- vertex_affines: float32 [6, 128, 256], P(None, ('sec', 'ty')), parts along dimension 1
The draws below stay inside these ranges and needn't reach their ends.
There are 2 independent parts, one for each index of `sec`. The reference program is written for one: setup_inputs(seed, part) draws one part's arguments, and reference() takes and returns one part's arrays. A program takes and returns all parts, laid end to end along the dimension named above; each array names one. Nothing has to cross between parts.
Inputs may be any that keep to these rules, and one draw needn't show every extreme that they name: `points`: for tile t, rows 0 and 1 are fixed positions: each 16 x 16 pixel cell of rows t*32 to (t+1)*32 and columns 0 to 2048 holds 4 of them, listed cell by cell, cells in row-major order; rows 2 and 3 are the matching moving positions. Source block j is rows j*16 to (j+1)*16 - 1. Tile t samples blocks slab_first[t] to slab_first[t] + slab_count[t] - 1, all within rows (t-1)*32 to (t+2)*32 - 1. slab_count reaches 6 on some tile in every draw.
All inputs are finite; a program needn't handle non-finite values.
Results may differ from the reference program's by a relative error of at most 0.008.
Values may be sent and summed in bfloat16 or wider, within the bound.
A program may use at most 64 MiB of HBM per device.

```python
import jax
import jax.numpy as jnp
from jax import lax

W = 2048
BH = 16
NB = 2
PC = 4
SP = 8
H = 32
K = 6
P_SIZE = 1024
VR = 4
VC = 256
ROWS = 512
N_TY = 16


def strip_shifts(key):
    first_key, second_key = jax.random.split(jax.random.fold_in(key, 31))
    strip_ids = jnp.arange(N_TY, dtype=jnp.int32)
    shifts = jax.random.randint(first_key, (N_TY,), -1, 2, dtype=jnp.int32)
    chosen = jax.random.randint(second_key, (), 1, N_TY - 2, dtype=jnp.int32)
    shifts = jnp.where(strip_ids == chosen, -1, jnp.where(strip_ids == chosen + 1, 1, shifts))
    shifts = jnp.where(strip_ids == 0, jnp.maximum(shifts, 0), shifts)
    shifts = jnp.where(strip_ids == N_TY - 1, jnp.minimum(shifts, 0), shifts)
    return shifts


def slab_bounds(key):
    shifts = strip_shifts(key)
    strip_ids = jnp.arange(N_TY, dtype=jnp.int32)
    from_above = jnp.concatenate([shifts[:1], shifts[:-1]])
    from_below = jnp.concatenate([shifts[1:], shifts[-1:]])
    lowest = jnp.minimum(jnp.minimum(from_above, shifts), from_below)
    highest = jnp.maximum(jnp.maximum(from_above, shifts), from_below)
    first_slab = jnp.maximum(0, jnp.maximum((strip_ids - 1) * NB, (strip_ids + lowest) * NB - 1))
    end_slab = jnp.minimum(N_TY * NB, jnp.minimum((strip_ids + 2) * NB, (strip_ids + 1 + highest) * NB + 1))
    return (first_slab, end_slab - first_slab)


def draw_slab_first(key, part):
    return slab_bounds(key)[0]


def draw_slab_count(key, part):
    return slab_bounds(key)[1]


def draw_points(key, part):
    shifts = strip_shifts(key).astype(jnp.float32)
    subkeys = jax.random.split(jax.random.fold_in(key, 57), 5)
    cell_cols = W // 16
    point_id = jnp.arange(N_TY * P_SIZE, dtype=jnp.int32)
    strip_id = point_id // P_SIZE
    cell_id = point_id % P_SIZE // PC
    base_x = (cell_id % cell_cols * 16).astype(jnp.float32)
    base_y = (strip_id * H + cell_id // cell_cols * 16).astype(jnp.float32)
    jitter = jax.random.uniform(subkeys[0], (2, N_TY * P_SIZE), minval=0.0, maxval=16.0)
    fixed_x = base_x + jitter[0]
    fixed_y = base_y + jitter[1]
    stretch = jax.random.uniform(subkeys[1], (N_TY,), minval=-0.03, maxval=0.03)
    sideways = jax.random.uniform(subkeys[2], (N_TY,), minval=-16.0, maxval=16.0)
    shear_y = jax.random.uniform(subkeys[3], (N_TY,), minval=-0.004, maxval=0.004)
    wobble = jnp.clip(jax.random.normal(subkeys[4], (2, N_TY * P_SIZE)), -3.0, 3.0)
    centre = W / 2.0
    moved_x = centre + (1.0 + stretch[strip_id]) * (fixed_x - centre) + sideways[strip_id] + wobble[0]
    moved_y = fixed_y + shifts[strip_id] * H + shear_y[strip_id] * (fixed_x - centre) + wobble[1]
    return jnp.stack([fixed_x, fixed_y, moved_x, moved_y]).astype(jnp.float32)


def block_scale(own_key, shape, cuts, low, high):
    gain = 1.0
    for dim, blocks in cuts:
        draws = jax.random.uniform(jax.random.fold_in(jax.random.fold_in(own_key, 6), dim), (blocks,), jnp.float32, low / len(cuts), high / len(cuts))
        gain = gain * jnp.repeat(jnp.exp(draws), shape[dim] // blocks).reshape((-1,) + (1,) * (len(shape) - 1 - dim))
    return gain


def bell_draw(own_key, extent, deviation, most, cuts=(), kind=jnp.bfloat16):
    drawn = deviation * jax.random.normal(own_key, extent, jnp.float32)
    if cuts:
        drawn = drawn * block_scale(own_key, extent, cuts, -0.22, 0.18)
    return jnp.clip(drawn, -most, most).astype(kind)


def setup_inputs(seed: int = 0, part: int = 0) -> dict:
    splits = jax.random.split(jax.random.key(seed), 5)
    part_splits = jax.random.split(jax.random.fold_in(splits[4], part), 5)
    points = draw_points(jax.random.fold_in(jax.random.fold_in(splits[4], part), 71), part)
    source = bell_draw(part_splits[1], (ROWS, W), 1.0, 4.0, ((0, 16),))
    slab_first = draw_slab_first(jax.random.fold_in(jax.random.fold_in(splits[4], part), 71), part)
    slab_count = draw_slab_count(jax.random.fold_in(jax.random.fold_in(splits[4], part), 71), part)
    return {"points": points, "source": source, "slab_first": slab_first, "slab_count": slab_count}


PRECISE = lax.Precision.HIGHEST
RIDGE_TERM = 0.01


def solve_affine(moments, vertex_x, vertex_y):
    mass = moments[0]
    mean_px = moments[1] / mass
    mean_py = moments[2] / mass
    mean_qx = moments[3] / mass
    mean_qy = moments[4] / mass
    cov_xx = moments[5] / mass - mean_px * mean_px + RIDGE_TERM
    cov_xy = moments[6] / mass - mean_px * mean_py
    cov_yy = moments[7] / mass - mean_py * mean_py + RIDGE_TERM
    cross_xx = moments[8] / mass - mean_qx * mean_px
    cross_xy = moments[9] / mass - mean_qx * mean_py
    cross_yx = moments[10] / mass - mean_qy * mean_px
    cross_yy = moments[11] / mass - mean_qy * mean_py
    determ = cov_xx * cov_yy - cov_xy * cov_xy
    lin_xx = (cross_xx * cov_yy - cross_xy * cov_xy) / determ
    lin_xy = (cross_xy * cov_xx - cross_xx * cov_xy) / determ
    lin_yx = (cross_yx * cov_yy - cross_yy * cov_xy) / determ
    lin_yy = (cross_yy * cov_xx - cross_yx * cov_xy) / determ
    delta_x = vertex_x - mean_px
    delta_y = vertex_y - mean_py
    shift_x = mean_qx + lin_xx * delta_x + lin_xy * delta_y - vertex_x
    shift_y = mean_qy + lin_yx * delta_x + lin_yy * delta_y - vertex_y
    return jnp.stack([lin_xx, lin_xy, lin_yx, lin_yy, shift_x, shift_y])


def block_moments(pts, usable, strip_id):
    block_count = W // 128
    per_block = VC // block_count
    cell_rows = pts.shape[1] // (block_count * 8 * PC)
    grid = pts.reshape(4, cell_rows, block_count, 8 * PC)
    live = usable.reshape(cell_rows, block_count, 8 * PC)
    grid = jnp.pad(grid, ((0, 0), (0, 0), (1, 1), (0, 0)))
    live = jnp.pad(live, ((0, 0), (1, 1), (0, 0)))
    near = jnp.concatenate([grid[:, :, 0:block_count], grid[:, :, 1:block_count + 1],
                            grid[:, :, 2:block_count + 2]], axis=3)
    near_live = jnp.concatenate([live[:, 0:block_count], live[:, 1:block_count + 1],
                                 live[:, 2:block_count + 2]], axis=2)
    near = jnp.transpose(near, (0, 2, 1, 3)).reshape(4, block_count, cell_rows * 24 * PC)
    near_live = jnp.transpose(near_live, (1, 0, 2)).reshape(block_count, cell_rows * 24 * PC)
    centre_y = strip_id.astype(jnp.float32) * H + H / 2.0
    anchor = jnp.arange(block_count, dtype=jnp.float32) * 128.0 + 64.0
    fixed_x = (near[0] - anchor[:, None]) / H
    fixed_y = (near[1] - centre_y) / H
    moved_x = (near[2] - anchor[:, None]) / H
    moved_y = (near[3] - centre_y) / H
    unit_row = jnp.ones_like(fixed_x)
    features = jnp.stack([unit_row, fixed_x, fixed_y, moved_x, moved_y, fixed_x * fixed_x, fixed_x * fixed_y,
                          fixed_y * fixed_y, moved_x * fixed_x, moved_x * fixed_y, moved_y * fixed_x,
                          moved_y * fixed_y], axis=1) * near_live[:, None, :]
    vertex_col = jnp.arange(VC, dtype=jnp.float32).reshape(block_count, per_block) * SP + SP / 2.0
    vertex_row = jnp.arange(VR, dtype=jnp.float32) * SP + SP / 2.0 - H / 2.0
    gap_x = (near[0][:, :, None] - vertex_col[:, None, :]) / H
    gap_y = fixed_y[:, :, None] - (vertex_row / H)[None, None, :]
    weight_x = jnp.exp(-2.0 * gap_x * gap_x)
    weight_y = jnp.exp(-2.0 * gap_y * gap_y)
    weighted = features[:, :, None, :] * jnp.transpose(weight_y, (0, 2, 1))[:, None, :, :]
    moments = jnp.einsum("bkrm,bmc->bkrc", weighted, weight_x, precision=PRECISE)
    return jnp.transpose(moments, (1, 2, 0, 3)).reshape(12, VR, VC)


def vertex_frame():
    block_count = W // 128
    per_block = VC // block_count
    anchor = jnp.arange(block_count, dtype=jnp.float32) * 128.0 + 64.0
    vertex_col = jnp.arange(VC, dtype=jnp.float32) * SP + SP / 2.0
    vertex_row = jnp.arange(VR, dtype=jnp.float32) * SP + SP / 2.0 - H / 2.0
    column_anchor = jnp.repeat(anchor, per_block)
    vertex_x = jnp.broadcast_to(((vertex_col - column_anchor) / H)[None, :], (VR, VC))
    vertex_y = jnp.broadcast_to((vertex_row / H)[:, None], (VR, VC))
    return vertex_x, vertex_y


def tent_tables():
    row_local = jnp.arange(H, dtype=jnp.float32)
    ext_row = (jnp.arange(VR + 2, dtype=jnp.float32) - 1.0) * SP + SP / 2.0
    tent_rows = jnp.maximum(0.0, 1.0 - jnp.abs(row_local[:, None] - ext_row[None, :]) / SP)
    column = jnp.clip(jnp.arange(W, dtype=jnp.float32), SP / 2.0, W - SP / 2.0)
    vertex_col = jnp.arange(VC, dtype=jnp.float32) * SP + SP / 2.0
    tent_cols = jnp.maximum(0.0, 1.0 - jnp.abs(column[None, :] - vertex_col[:, None]) / SP)
    return tent_rows, tent_cols


def displace(near_shift, tent_rows, tent_cols):
    first_part = jnp.dot(jnp.dot(tent_rows, near_shift[0], precision=PRECISE), tent_cols, precision=PRECISE)
    second_part = jnp.dot(jnp.dot(tent_rows, near_shift[1], precision=PRECISE), tent_cols, precision=PRECISE)
    return jnp.stack([first_part, second_part])


def render_strip(slab_rows, first_slab, slab_total, disp, strip_id):
    block_count = W // 128
    samp_y = jnp.arange(H, dtype=jnp.float32)[:, None] + H * disp[1]
    samp_x = jnp.arange(W, dtype=jnp.float32)[None, :] + H * disp[0]
    slot_ids = jnp.arange(K, dtype=jnp.int32)
    slot_row = (first_slab + slot_ids) * BH - strip_id * H
    row_pos = (slot_row[:, None] + jnp.arange(BH, dtype=jnp.int32)[None, :]).reshape(K * BH).astype(jnp.float32)
    slot_live = jnp.repeat((slot_ids < slab_total).astype(jnp.float32), BH)
    padded = jnp.pad(slab_rows, ((0, 0), (64, 192)))
    blocks = padded.reshape(K * BH, block_count + 2, 128)
    windows = jnp.concatenate([blocks[:, :block_count], blocks[:, 1:block_count + 1]], axis=2)
    windows = jnp.transpose(windows, (1, 0, 2))
    block_y = samp_y.reshape(H, block_count, 128).transpose(1, 0, 2).reshape(block_count, H * 128)
    block_x = samp_x.reshape(H, block_count, 128).transpose(1, 0, 2).reshape(block_count, H * 128)
    block_ids = jnp.arange(block_count, dtype=jnp.int32)

    def one_block(packed):
        along_y, along_x, window, block_id = packed
        col_pos = block_id.astype(jnp.float32) * 128.0 - 64.0 + jnp.arange(256, dtype=jnp.float32)
        across = jnp.maximum(0.0, 1.0 - jnp.abs(along_x[:, None] - col_pos[None, :])).astype(jnp.bfloat16)
        mixed_rows = jnp.dot(across.astype(jnp.float32), jnp.transpose(window.astype(jnp.float32)), precision=PRECISE)
        tent_y = jnp.maximum(0.0, 1.0 - jnp.abs(along_y[:, None] - row_pos[None, :])) * slot_live
        return jnp.sum(mixed_rows * tent_y, axis=1)

    pieces = lax.map(one_block, (block_y, block_x, windows, block_ids))
    return pieces.reshape(block_count, H, 128).transpose(1, 0, 2).reshape(H, W).astype(jnp.bfloat16)


def reference(points, source, slab_first, slab_count):
    strip_ids = jnp.arange(N_TY, dtype=jnp.int32)
    padded_pts = jnp.pad(points, ((0, 0), (P_SIZE, P_SIZE)))
    vertex_x, vertex_y = vertex_frame()

    def fit_strip(strip_id):
        nearby = lax.dynamic_slice_in_dim(padded_pts, strip_id * P_SIZE, 3 * P_SIZE, 1)
        owners = strip_id - 1 + jnp.arange(3 * P_SIZE, dtype=jnp.int32) // P_SIZE
        usable = ((owners >= 0) & (owners < N_TY)).astype(jnp.float32)
        return solve_affine(block_moments(nearby, usable, strip_id), vertex_x, vertex_y)

    affines = lax.map(fit_strip, strip_ids)
    vertex_affines = jnp.transpose(affines, (1, 0, 2, 3)).reshape(6, N_TY * VR, VC)
    flat_shift = vertex_affines[4:6]
    extended = jnp.concatenate([flat_shift[:, :1], flat_shift, flat_shift[:, -1:]], axis=1)
    source_pad = jnp.pad(source, ((0, K * BH), (0, 0)))
    tent_rows, tent_cols = tent_tables()

    def render_one(strip_id):
        near_shift = lax.dynamic_slice_in_dim(extended, strip_id * VR, VR + 2, 1)
        disp = displace(near_shift, tent_rows, tent_cols)
        first_slab = slab_first[strip_id]
        slab_total = slab_count[strip_id]
        slab_rows = lax.dynamic_slice_in_dim(source_pad, (first_slab * BH).astype(jnp.int32), K * BH, 0)
        return render_strip(slab_rows, first_slab, slab_total, disp, strip_id)

    rendered = lax.map(render_one, strip_ids).reshape(N_TY * H, W)
    return rendered, vertex_affines
```

```python
import jax
import jax.numpy as jnp
from jax import lax
from jax.experimental import pallas as pl
from jax.experimental.pallas import tpu as pltpu
from jax.sharding import PartitionSpec as P

W = 2048
BH = 16
SP = 8
H = 32
K = 6
VR = 4
VC = 256


MESH = pl.DeviceIdType.MESH
RIDGE_TERM = 0.01


def solve_affine(moments, vertex_x, vertex_y):
    mass = moments[0]
    mean_px = moments[1] / mass
    mean_py = moments[2] / mass
    mean_qx = moments[3] / mass
    mean_qy = moments[4] / mass
    cov_xx = moments[5] / mass - mean_px * mean_px + RIDGE_TERM
    cov_xy = moments[6] / mass - mean_px * mean_py
    cov_yy = moments[7] / mass - mean_py * mean_py + RIDGE_TERM
    cross_xx = moments[8] / mass - mean_qx * mean_px
    cross_xy = moments[9] / mass - mean_qx * mean_py
    cross_yx = moments[10] / mass - mean_qy * mean_px
    cross_yy = moments[11] / mass - mean_qy * mean_py
    determ = cov_xx * cov_yy - cov_xy * cov_xy
    lin_xx = (cross_xx * cov_yy - cross_xy * cov_xy) / determ
    lin_xy = (cross_xy * cov_xx - cross_xx * cov_xy) / determ
    lin_yx = (cross_yx * cov_yy - cross_yy * cov_xy) / determ
    lin_yy = (cross_yy * cov_xx - cross_yx * cov_xy) / determ
    delta_x = vertex_x - mean_px
    delta_y = vertex_y - mean_py
    shift_x = mean_qx + lin_xx * delta_x + lin_xy * delta_y - vertex_x
    shift_y = mean_qy + lin_yx * delta_x + lin_yy * delta_y - vertex_y
    return [lin_xx, lin_xy, lin_yx, lin_yy, shift_x, shift_y]


OFFSETS = (1, -1, 2, -2)


def fit_kernel(pts_ref, src_ref, fit_ref, wide,
               held, staged, mom, send_p, recv_p, send_s, recv_s, load):
    f32 = jnp.float32
    me = lax.axis_index("ty")
    n = lax.axis_size("ty")
    size = pts_ref.shape[1]
    half = size // 2
    pairs = W // 256

    def exists(d):
        return (me + d >= 0) & (me + d < n)

    own_points = pltpu.make_async_copy(pts_ref, held.at[2], load)
    own_points.start()
    barrier = pltpu.get_barrier_semaphore()
    for d in OFFSETS:
        @pl.when(exists(d))
        def _(d=d):
            pl.semaphore_signal(barrier, inc=1, device_id={"ty": me + d}, device_id_type=MESH)
    peers = sum(exists(d).astype(jnp.int32) for d in OFFSETS)
    pl.semaphore_wait(barrier, peers)
    own_points.wait()

    def points_to(i, d):
        return pltpu.make_async_remote_copy(
            src_ref=held.at[2], dst_ref=held.at[2 - d], send_sem=send_p.at[i], recv_sem=recv_p.at[i],
            device_id={"ty": me + d}, device_id_type=MESH)

    def source_to(i, d):
        return pltpu.make_async_remote_copy(
            src_ref=src_ref, dst_ref=wide.at[i], send_sem=send_s.at[i], recv_sem=recv_s.at[i],
            device_id={"ty": me + d}, device_id_type=MESH)

    for i, d in enumerate(OFFSETS):
        @pl.when(exists(d))
        def _(i=i, d=d):
            points_to(i, d).start()
    for i, d in enumerate(OFFSETS[:2]):
        @pl.when(exists(d))
        def _(i=i, d=d):
            source_to(i, d).start()
    for i, d in enumerate(OFFSETS):
        @pl.when(exists(-d))
        def _(i=i, d=d):
            points_to(i, d).wait_recv()

    spare = jnp.zeros((4, 128), f32)
    for tile in range(5):
        data = held[2] if tile == 2 else jnp.where(exists(tile - 2), held[tile], 0.0)
        for c in range(2):
            row = jnp.concatenate([data[:, c * half : (c + 1) * half], spare], axis=1)
            staged[0, 2 * tile + c] = pltpu.roll(row, 32, 1)
            staged[1, 2 * tile + c] = pltpu.roll(row, half + 96, 1)

    e = lax.broadcasted_iota(jnp.int32, (8, 128), 0)
    own = jnp.where(e == 0, 1, jnp.where(e == 5, 3, 2))
    vy = (((e - 1) * SP + SP // 2) - H // 2).astype(f32) * (1.0 / H)
    lane32 = lax.broadcasted_iota(jnp.int32, (32, 128), 1)
    vert32 = lax.broadcasted_iota(jnp.int32, (32, 128), 0)
    vx32 = (vert32 * SP + SP // 2 - 128).astype(f32) * (1.0 / H)
    centre = (me * H).astype(f32) + H / 2.0

    def group(k, _):
        for odd in range(2):
            pair = 2 * k + odd
            anchor = (pair * 256 + 128).astype(f32)
            block = 2 * pair - 1 + lane32 // 32
            mine = 2 * pair + vert32 // 16
            near = (jnp.abs(block - mine) <= 1) & (block >= 0) & (block < 2 * pairs)
            parts, weights = [], []
            for t in range(10):
                tile = t // 2
                box = staged[odd, t, :, pl.ds(pl.multiple_of(k * 128, 128), 128)]
                px = (box[0:1] - anchor) * (1.0 / H)
                py = (box[1:2] - centre) * (1.0 / H)
                qx = (box[2:3] - anchor) * (1.0 / H)
                qy = (box[3:4] - centre) * (1.0 / H)
                gap = px - vx32
                across = jnp.where(near, jnp.exp(-2.0 * gap * gap), 0.0)
                near_part = across.astype(jnp.bfloat16)
                rest_part = (across - near_part.astype(f32)).astype(jnp.bfloat16)
                weights.append(jnp.concatenate([near_part, rest_part], axis=0))
                rise = py - vy
                there = (jnp.abs(own - tile) <= 1) & exists(tile - 2)
                w = jnp.where(there, jnp.exp(-2.0 * rise * rise), 0.0)
                wpx = w * px
                wpy = w * py
                feats = jnp.concatenate(
                    [w, wpx, wpy, w * qx, w * qy, wpx * px, wpx * py, wpy * py,
                     wpx * qx, wpy * qx, wpx * qy, wpy * qy], axis=0)
                high = feats.astype(jnp.bfloat16)
                low = (feats - high.astype(f32)).astype(jnp.bfloat16)
                parts.append(jnp.concatenate([high, low], axis=0))
            got = lax.dot_general(
                jnp.concatenate(parts, axis=1), jnp.concatenate(weights, axis=1),
                (((1,), (1,)), ((), ())), preferred_element_type=f32)
            got = got[0:96] + got[96:192]
            mom[pair] = got[:, 0:32] + got[:, 32:64]
        return 0

    lax.fori_loop(0, pairs // 2, group, 0)
    moments = [
        jnp.concatenate([mom[g, 8 * f : 8 * f + 8, :] for g in range(pairs)], axis=1) for f in range(12)
    ]
    ew = lax.broadcasted_iota(jnp.int32, (8, VC), 0)
    jw = lax.broadcasted_iota(jnp.int32, (8, VC), 1)
    vertex_y = (((ew - 1) * SP + SP // 2) - H // 2).astype(f32) * (1.0 / H)
    vertex_x = ((jw % 32) * SP + SP // 2 - 128).astype(f32) * (1.0 / H)
    safe = ew < 6
    moments[0] = jnp.where(safe, moments[0], 1.0)
    solved = solve_affine(moments, vertex_x, vertex_y)
    for f in range(6):
        x = solved[f]
        if f >= 4:
            x = jnp.where((ew == 0) & (me == 0), x[1:2], x)
            x = jnp.where((ew == 5) & (me == n - 1), x[4:5], x)
            x = jnp.where(safe, x, 0.0)
        fit_ref[8 * f : 8 * f + 8, :] = x

    for i, d in enumerate(OFFSETS[:2]):
        @pl.when(exists(-d))
        def _(i=i, d=d):
            source_to(i, d).wait_recv()
    for i, d in enumerate(OFFSETS):
        @pl.when(exists(d))
        def _(i=i, d=d):
            points_to(i, d).wait_send()
    for i, d in enumerate(OFFSETS[:2]):
        @pl.when(exists(d))
        def _(i=i, d=d):
            source_to(i, d).wait_send()


def fit(points, source):
    size = points.shape[1]
    vm = pl.BlockSpec(memory_space=pltpu.VMEM)
    return pl.pallas_call(
        fit_kernel,
        out_shape=(
            jax.ShapeDtypeStruct((48, VC), jnp.float32),
            jax.ShapeDtypeStruct((2, H, W), jnp.bfloat16),
        ),
        in_specs=[pl.BlockSpec(memory_space=pl.ANY)] * 2,
        out_specs=(vm, pl.BlockSpec(memory_space=pl.ANY)),
        scratch_shapes=[
            pltpu.VMEM((5, 4, size), jnp.float32),
            pltpu.VMEM((2, 10, 4, size // 2 + 128), jnp.float32),
            pltpu.VMEM((W // 256, 96, 32), jnp.float32),
            pltpu.SemaphoreType.DMA((4,)),
            pltpu.SemaphoreType.DMA((4,)),
            pltpu.SemaphoreType.DMA((2,)),
            pltpu.SemaphoreType.DMA((2,)),
            pltpu.SemaphoreType.DMA,
        ],
        compiler_params=pltpu.CompilerParams(collective_id=0, has_side_effects=True),
        name="fit",
    )(points, source)


GROUPS = H // SP
FIRST = 4
MORE = 2
PER = 7


def pick(x, lanes):
    dims = lax.GatherDimensionNumbers(
        offset_dims=(), collapsed_slice_dims=(1,), start_index_map=(1,),
        operand_batching_dims=(0,), start_indices_batching_dims=(0,))
    return lax.gather(x, lanes[..., None], dims, slice_sizes=(1, 1),
                      mode=lax.GatherScatterMode.PROMISE_IN_BOUNDS)


def render_kernel(first_ref, count_ref, fit_ref, own_ref, wide_ref, out_ref, aff_ref,
                  src_ref, pages, ext, sp_s, low_s, ix_s, w0_s, w1_s, num_v, num_m, first_m, count_m, sems):
    blocks = W // 128
    tile = lax.axis_index("ty")
    n = lax.axis_size("ty")
    f32 = jnp.float32
    scalars = [
        pltpu.make_async_copy(first_ref, first_m, sems.at[0]),
        pltpu.make_async_copy(count_ref, count_m, sems.at[1]),
    ]
    for c in scalars:
        c.start()
    own = pltpu.make_async_copy(own_ref, src_ref.at[pl.ds(H, H)], sems.at[2])
    own.start()
    sides = [
        (tile > 0, 0, pltpu.make_async_copy(wide_ref.at[0], src_ref.at[pl.ds(0, H)], sems.at[3])),
        (tile < n - 1, 2 * H, pltpu.make_async_copy(wide_ref.at[1], src_ref.at[pl.ds(2 * H, H)], sems.at[4])),
    ]
    for there, at, c in sides:
        @pl.when(there)
        def _(c=c):
            c.start()

        @pl.when(jnp.logical_not(there))
        def _(at=at):
            src_ref[at : at + H, :] = jnp.zeros((H, W), jnp.bfloat16)
    for f in range(6):
        aff_ref[f] = fit_ref[8 * f + 1 : 8 * f + 5, :]

    left, right = fit_ref[32:48, 0:128], fit_ref[32:48, 128:256]
    lane16 = lax.broadcasted_iota(jnp.int32, (16, 128), 1)
    ext[0] = jnp.where(lane16 < 1, left[:, 0:1], pltpu.roll(left, 1, 1))
    ext[1] = jnp.where(lane16 < 17, pltpu.roll(left, 17, 1), pltpu.roll(right, 17, 1))
    ext[2] = jnp.where(lane16 < 33, pltpu.roll(right, 33, 1), right[:, 127:128])

    sub = lax.broadcasted_iota(jnp.int32, (8, 128), 0)
    subf = sub.astype(f32)
    lane = lax.broadcasted_iota(jnp.int32, (8, 128), 1)
    wa = jnp.maximum(0.0, 1.0 - (subf + 4.0) * (1.0 / SP))
    wb = jnp.maximum(0.0, 1.0 - jnp.abs(subf - 4.0) * (1.0 / SP))
    wc = jnp.maximum(0.0, 1.0 - (12.0 - subf) * (1.0 / SP))
    lanef = lane.astype(f32)
    step = (lane + SP // 2) // SP
    part = ((lane + SP // 2) % SP).astype(f32) * (1.0 / SP)

    def prepare(b, spans):
        page = b // PER
        at = step + (b - page * PER) * (128 // SP)
        fine = []
        for half in range(2):
            held = ext[page, 8 * half : 8 * half + 8, :]
            near = pick(held, at)
            fine.append(near + part * (pick(held, at + 1) - near))
        fx, fy = fine
        most = None
        for g in range(GROUPS):
            dx = wa * fx[g : g + 1] + wb * fx[g + 1 : g + 2] + wc * fx[g + 2 : g + 3]
            dy = wa * fy[g : g + 1] + wb * fy[g + 1 : g + 2] + wc * fy[g + 2 : g + 3]
            sy = jnp.clip(subf + (8.0 * g) + H * dy, -33.0, 64.0)
            sx = (lanef + (b * 128).astype(f32)) + H * dx
            lx = jnp.clip(sx - (b * 128 - 64).astype(f32), -1.0, 256.0)
            base = jnp.floor(lx)
            frac = lx - base
            ix = base.astype(jnp.int32)
            w0 = jnp.where(ix < 0, frac, jnp.where(ix < 256, 1.0 - frac, 0.0)).astype(jnp.bfloat16).astype(f32)
            w1 = jnp.where((ix >= 0) & (ix < 255), frac, 0.0).astype(jnp.bfloat16).astype(f32)
            r = slice(8 * g, 8 * g + 8)
            low = jnp.floor(jnp.min(sy, axis=1, keepdims=True))
            rel = sy - low
            most = rel if most is None else jnp.maximum(most, rel)
            sp_s[b, r, :] = rel
            low_s[b, r, :] = jnp.broadcast_to(low, (8, 128))
            ix_s[b, r, :] = jnp.clip(ix, 0, 255)
            w0_s[b, r, :] = w0
            w1_s[b, r, :] = w1
        return jnp.where(lane == b, jnp.max(most, axis=1, keepdims=True), spans)

    spans = lax.fori_loop(0, blocks, prepare, jnp.zeros((8, 128), f32))
    rows = jnp.floor(jnp.max(spans, axis=0, keepdims=True)).astype(jnp.int32) + 2
    extra = (jnp.maximum(rows - FIRST, 0) + (MORE - 1)) // MORE
    num_v[...] = jnp.broadcast_to(extra, (8, 128))
    bring = pltpu.make_async_copy(num_v, num_m, sems.at[5])
    bring.start()

    own.wait()
    for there, _, c in sides:
        @pl.when(there)
        def _(c=c):
            c.wait()
    lanes = lax.broadcasted_iota(jnp.int32, (3 * H, 128), 1)
    zero = jnp.zeros((3 * H, 128), jnp.bfloat16)
    prev = zero
    for k in range(blocks + 1):
        now = pltpu.roll(src_ref[:, 128 * k : 128 * k + 128], 64, 1) if k < blocks else zero
        pages[:, 128 * k : 128 * k + 128] = jnp.where(lanes < 64, prev, now)
        prev = now

    for c in scalars:
        c.wait()
    first = first_m[0] * BH - tile * H + H
    last = first + count_m[0] * BH
    slot = lax.broadcasted_iota(jnp.int32, (8, 3 * H), 1)
    slot = jnp.where((slot >= first) & (slot < last), (slot - H).astype(f32), -1e6)
    bring.wait()

    def paint(b, _):
        window = pages[:, pl.ds(pl.multiple_of(b * 128, 128), 256)]
        lows = [low_s[b, 8 * g : 8 * g + 8, :][:, : 3 * H] for g in range(GROUPS)]
        taps, weights, rel = [], [], []
        for g in range(GROUPS):
            i0 = ix_s[b, 8 * g : 8 * g + 8, :]
            i1 = i0 + 1
            taps.append([(i < 128, i & 127) for i in (i0, i1)])
            weights.append((w0_s[b, 8 * g : 8 * g + 8, :], w1_s[b, 8 * g : 8 * g + 8, :]))
            rel.append(sp_s[b, 8 * g : 8 * g + 8, :])

        def chunk(start, size, accs):
            offs = [start + d for d in range(size)]
            onehot = jnp.concatenate(
                [jnp.where(slot == lows[g] + o, 1.0, 0.0) for g in range(GROUPS) for o in offs], axis=0)
            got = jnp.dot(onehot.astype(jnp.bfloat16), window, preferred_element_type=f32)
            out = []
            for g in range(GROUPS):
                acc = accs[g]
                for d in range(size):
                    at = 8 * (g * size + d)
                    near, far = got[at : at + 8, :128], got[at : at + 8, 128:]
                    mixed = sum(
                        jnp.where(here, pick(near, m), pick(far, m)) * w
                        for (here, m), w in zip(taps[g], weights[g]))
                    term = mixed * jnp.maximum(0.0, 1.0 - jnp.abs(rel[g] - offs[d]))
                    acc = term if acc is None else acc + term
                out.append(acc)
            return tuple(out)

        accs = chunk(0.0, FIRST, (None,) * GROUPS)

        def more(k, accs):
            return chunk((FIRST + MORE * k).astype(f32), MORE, accs)

        accs = lax.fori_loop(0, num_m[0, b], more, accs)
        out_ref[:, pl.ds(pl.multiple_of(b * 128, 128), 128)] = jnp.concatenate(accs, axis=0).astype(jnp.bfloat16)
        return 0

    lax.fori_loop(0, blocks, paint, 0)


def render(first, count, fitted, source, wide):
    blocks = W // 128
    vm = pl.BlockSpec(memory_space=pltpu.VMEM)
    hbm = pl.BlockSpec(memory_space=pl.ANY)
    per = lambda d: pltpu.VMEM((blocks, H, 128), d)
    return pl.pallas_call(
        render_kernel,
        out_shape=(
            jax.ShapeDtypeStruct((H, W), jnp.bfloat16),
            jax.ShapeDtypeStruct((6, VR, VC), jnp.float32),
        ),
        in_specs=[hbm, hbm, vm, hbm, hbm],
        out_specs=(vm, vm),
        scratch_shapes=[
            pltpu.VMEM((3 * H, W), jnp.bfloat16),
            pltpu.VMEM((3 * H, W + 128), jnp.bfloat16),
            pltpu.VMEM((-(-blocks // PER), 16, 128), jnp.float32),
            per(jnp.float32), per(jnp.float32), per(jnp.int32), per(jnp.float32), per(jnp.float32),
            pltpu.VMEM((8, 128), jnp.int32),
            pltpu.SMEM((8, 128), jnp.int32),
            pltpu.SMEM((1,), jnp.int32),
            pltpu.SMEM((1,), jnp.int32),
            pltpu.SemaphoreType.DMA((6,)),
        ],
        name="render",
    )(first, count, fitted, source, wide)


def per_device(points, source, slab_first, slab_count):
    fitted, wide = fit(points, source)
    rendered, affines = render(slab_first, slab_count, fitted, source, wide)
    return (rendered, affines)


def solution(mesh):
    return jax.shard_map(
        per_device,
        mesh=mesh,
        in_specs=(
            P(None, ("sec", "ty")),
            P(("sec", "ty"), None),
            P(("sec", "ty")),
            P(("sec", "ty")),
        ),
        out_specs=(P(("sec", "ty"), None), P(None, ("sec", "ty"), None)),
        check_vma=False,
    )
```

```python
import jax
import jax.numpy as jnp
from jax import lax
from jax.experimental import pallas as pl
from jax.experimental.pallas import tpu as pltpu
from jax.sharding import PartitionSpec as P

W = 2048
BH = 16
SP = 8
H = 32
K = 6
VR = 4
VC = 256


MESH = pl.DeviceIdType.MESH
RIDGE_TERM = 0.01


def solve_affine(moments, vertex_x, vertex_y):
    mass = moments[0]
    mean_px = moments[1] / mass
    mean_py = moments[2] / mass
    mean_qx = moments[3] / mass
    mean_qy = moments[4] / mass
    cov_xx = moments[5] / mass - mean_px * mean_px + RIDGE_TERM
    cov_xy = moments[6] / mass - mean_px * mean_py
    cov_yy = moments[7] / mass - mean_py * mean_py + RIDGE_TERM
    cross_xx = moments[8] / mass - mean_qx * mean_px
    cross_xy = moments[9] / mass - mean_qx * mean_py
    cross_yx = moments[10] / mass - mean_qy * mean_px
    cross_yy = moments[11] / mass - mean_qy * mean_py
    determ = cov_xx * cov_yy - cov_xy * cov_xy
    lin_xx = (cross_xx * cov_yy - cross_xy * cov_xy) / determ
    lin_xy = (cross_xy * cov_xx - cross_xx * cov_xy) / determ
    lin_yx = (cross_yx * cov_yy - cross_yy * cov_xy) / determ
    lin_yy = (cross_yy * cov_xx - cross_yx * cov_xy) / determ
    delta_x = vertex_x - mean_px
    delta_y = vertex_y - mean_py
    shift_x = mean_qx + lin_xx * delta_x + lin_xy * delta_y - vertex_x
    shift_y = mean_qy + lin_yx * delta_x + lin_yy * delta_y - vertex_y
    return [lin_xx, lin_xy, lin_yx, lin_yy, shift_x, shift_y]


OFFSETS = (1, -1, 2, -2)


def fit_kernel(pts_ref, src_ref, fit_ref, wide,
               held, staged, mom, send_p, recv_p, send_s, recv_s, load):
    f32 = jnp.float32
    me = lax.axis_index("ty")
    n = lax.axis_size("ty")
    size = pts_ref.shape[1]
    half = size // 2
    pairs = W // 256

    def exists(d):
        return (me + d >= 0) & (me + d < n)

    own_points = pltpu.make_async_copy(pts_ref, held.at[2], load)
    own_points.start()
    barrier = pltpu.get_barrier_semaphore()
    for d in OFFSETS:
        @pl.when(exists(d))
        def _(d=d):
            pl.semaphore_signal(barrier, inc=1, device_id={"ty": me + d}, device_id_type=MESH)
    peers = sum(exists(d).astype(jnp.int32) for d in OFFSETS)
    pl.semaphore_wait(barrier, peers)
    own_points.wait()

    def points_to(i, d):
        return pltpu.make_async_remote_copy(
            src_ref=held.at[2], dst_ref=held.at[2 - d], send_sem=send_p.at[i], recv_sem=recv_p.at[i],
            device_id={"ty": me + d}, device_id_type=MESH)

    def source_to(i, d):
        return pltpu.make_async_remote_copy(
            src_ref=src_ref, dst_ref=wide.at[i], send_sem=send_s.at[i], recv_sem=recv_s.at[i],
            device_id={"ty": me + d}, device_id_type=MESH)

    for i, d in enumerate(OFFSETS):
        @pl.when(exists(d))
        def _(i=i, d=d):
            points_to(i, d).start()
    for i, d in enumerate(OFFSETS[:2]):
        @pl.when(exists(d))
        def _(i=i, d=d):
            source_to(i, d).start()
    for i, d in enumerate(OFFSETS):
        @pl.when(exists(-d))
        def _(i=i, d=d):
            points_to(i, d).wait_recv()

    spare = jnp.zeros((4, 128), f32)
    for tile in range(5):
        data = held[2] if tile == 2 else jnp.where(exists(tile - 2), held[tile], 0.0)
        for c in range(2):
            row = jnp.concatenate([data[:, c * half : (c + 1) * half], spare], axis=1)
            staged[0, 2 * tile + c] = pltpu.roll(row, 32, 1)
            staged[1, 2 * tile + c] = pltpu.roll(row, half + 96, 1)

    e = lax.broadcasted_iota(jnp.int32, (8, 128), 0)
    own = jnp.where(e == 0, 1, jnp.where(e == 5, 3, 2))
    vy = (((e - 1) * SP + SP // 2) - H // 2).astype(f32) * (1.0 / H)
    lane32 = lax.broadcasted_iota(jnp.int32, (32, 128), 1)
    vert32 = lax.broadcasted_iota(jnp.int32, (32, 128), 0)
    vx32 = (vert32 * SP + SP // 2 - 128).astype(f32) * (1.0 / H)
    centre = (me * H).astype(f32) + H / 2.0

    def group(k, _):
        for odd in range(2):
            pair = 2 * k + odd
            anchor = (pair * 256 + 128).astype(f32)
            block = 2 * pair - 1 + lane32 // 32
            mine = 2 * pair + vert32 // 16
            near = (jnp.abs(block - mine) <= 1) & (block >= 0) & (block < 2 * pairs)
            parts, weights = [], []
            for t in range(10):
                tile = t // 2
                box = staged[odd, t, :, pl.ds(pl.multiple_of(k * 128, 128), 128)]
                px = (box[0:1] - anchor) * (1.0 / H)
                py = (box[1:2] - centre) * (1.0 / H)
                qx = (box[2:3] - anchor) * (1.0 / H)
                qy = (box[3:4] - centre) * (1.0 / H)
                gap = px - vx32
                across = jnp.where(near, jnp.exp(-2.0 * gap * gap), 0.0)
                near_part = across.astype(jnp.bfloat16)
                rest_part = (across - near_part.astype(f32)).astype(jnp.bfloat16)
                weights.append(jnp.concatenate([near_part, rest_part], axis=0))
                rise = py - vy
                there = (jnp.abs(own - tile) <= 1) & exists(tile - 2)
                w = jnp.where(there, jnp.exp(-2.0 * rise * rise), 0.0)
                wpx = w * px
                wpy = w * py
                feats = jnp.concatenate(
                    [w, wpx, wpy, w * qx, w * qy, wpx * px, wpx * py, wpy * py,
                     wpx * qx, wpy * qx, wpx * qy, wpy * qy], axis=0)
                high = feats.astype(jnp.bfloat16)
                low = (feats - high.astype(f32)).astype(jnp.bfloat16)
                parts.append(jnp.concatenate([high, low], axis=0))
            got = lax.dot_general(
                jnp.concatenate(parts, axis=1), jnp.concatenate(weights, axis=1),
                (((1,), (1,)), ((), ())), preferred_element_type=f32)
            got = got[0:96] + got[96:192]
            mom[pair] = got[:, 0:32] + got[:, 32:64]
        return 0

    lax.fori_loop(0, pairs // 2, group, 0)
    moments = [
        jnp.concatenate([mom[g, 8 * f : 8 * f + 8, :] for g in range(pairs)], axis=1) for f in range(12)
    ]
    ew = lax.broadcasted_iota(jnp.int32, (8, VC), 0)
    jw = lax.broadcasted_iota(jnp.int32, (8, VC), 1)
    vertex_y = (((ew - 1) * SP + SP // 2) - H // 2).astype(f32) * (1.0 / H)
    vertex_x = ((jw % 32) * SP + SP // 2 - 128).astype(f32) * (1.0 / H)
    safe = ew < 6
    moments[0] = jnp.where(safe, moments[0], 1.0)
    solved = solve_affine(moments, vertex_x, vertex_y)
    for f in range(6):
        x = solved[f]
        if f >= 4:
            x = jnp.where((ew == 0) & (me == 0), x[1:2], x)
            x = jnp.where((ew == 5) & (me == n - 1), x[4:5], x)
            x = jnp.where(safe, x, 0.0)
        fit_ref[8 * f : 8 * f + 8, :] = x

    for i, d in enumerate(OFFSETS[:2]):
        @pl.when(exists(-d))
        def _(i=i, d=d):
            source_to(i, d).wait_recv()
    for i, d in enumerate(OFFSETS):
        @pl.when(exists(d))
        def _(i=i, d=d):
            points_to(i, d).wait_send()
    for i, d in enumerate(OFFSETS[:2]):
        @pl.when(exists(d))
        def _(i=i, d=d):
            source_to(i, d).wait_send()


def fit(points, source):
    size = points.shape[1]
    vm = pl.BlockSpec(memory_space=pltpu.VMEM)
    return pl.pallas_call(
        fit_kernel,
        out_shape=(
            pltpu.VMEM((48, VC), jnp.float32),
            pltpu.VMEM((2, H, W), jnp.bfloat16),
        ),
        in_specs=[pl.BlockSpec(memory_space=pltpu.HBM)] * 2,
        out_specs=(vm, vm),
        scratch_shapes=[
            pltpu.VMEM((5, 4, size), jnp.float32),
            pltpu.VMEM((2, 10, 4, size // 2 + 128), jnp.float32),
            pltpu.VMEM((W // 256, 96, 32), jnp.float32),
            pltpu.SemaphoreType.DMA((4,)),
            pltpu.SemaphoreType.DMA((4,)),
            pltpu.SemaphoreType.DMA((2,)),
            pltpu.SemaphoreType.DMA((2,)),
            pltpu.SemaphoreType.DMA,
        ],
        compiler_params=pltpu.CompilerParams(collective_id=0, has_side_effects=True, vmem_limit_bytes=8 << 20),
        name="fit",
    )(points, source)


GROUPS = H // SP
FIRST = 8
UB = 4
UP = 4
MORE = 2
PER = 7


def pick(x, lanes):
    dims = lax.GatherDimensionNumbers(
        offset_dims=(), collapsed_slice_dims=(1,), start_index_map=(1,),
        operand_batching_dims=(0,), start_indices_batching_dims=(0,))
    return lax.gather(x, lanes[..., None], dims, slice_sizes=(1, 1),
                      mode=lax.GatherScatterMode.PROMISE_IN_BOUNDS)


def render_kernel(first_ref, count_ref, fit_ref, own_ref, wide_ref, out_ref, aff_ref,
                  src_ref, pages, pages1, ext, sp_s, low_s, ix_s, w0_s, w1_s, accum, num_v, num_m, sems):
    blocks = W // 128
    tile = lax.axis_index("ty")
    n = lax.axis_size("ty")
    f32 = jnp.float32
    own = pltpu.make_async_copy(own_ref, src_ref, sems.at[2])
    own.start()
    for f in range(6):
        aff_ref[f] = fit_ref[8 * f + 1 : 8 * f + 5, :]

    left, right = fit_ref[32:48, 0:128], fit_ref[32:48, 128:256]
    lane16 = lax.broadcasted_iota(jnp.int32, (16, 128), 1)
    ext[0] = jnp.where(lane16 < 1, left[:, 0:1], pltpu.roll(left, 1, 1))
    ext[1] = jnp.where(lane16 < 17, pltpu.roll(left, 17, 1), pltpu.roll(right, 17, 1))
    ext[2] = jnp.where(lane16 < 33, pltpu.roll(right, 33, 1), right[:, 127:128])

    sub = lax.broadcasted_iota(jnp.int32, (8, 128), 0)
    subf = sub.astype(f32)
    lane = lax.broadcasted_iota(jnp.int32, (8, 128), 1)
    wa = jnp.maximum(0.0, 1.0 - (subf + 4.0) * (1.0 / SP))
    wb = jnp.maximum(0.0, 1.0 - jnp.abs(subf - 4.0) * (1.0 / SP))
    wc = jnp.maximum(0.0, 1.0 - (12.0 - subf) * (1.0 / SP))
    lanef = lane.astype(f32)
    step = (lane + SP // 2) // SP
    part = ((lane + SP // 2) % SP).astype(f32) * (1.0 / SP)

    def prepare(b, spans):
        page = b // PER
        at = step + (b - page * PER) * (128 // SP)
        fine = []
        for half in range(2):
            held = ext[page, 8 * half : 8 * half + 8, :]
            near = pick(held, at)
            fine.append(near + part * (pick(held, at + 1) - near))
        fx, fy = fine
        most = None
        for g in range(GROUPS):
            dx = wa * fx[g : g + 1] + wb * fx[g + 1 : g + 2] + wc * fx[g + 2 : g + 3]
            dy = wa * fy[g : g + 1] + wb * fy[g + 1 : g + 2] + wc * fy[g + 2 : g + 3]
            sy = jnp.clip(subf + (8.0 * g) + H * dy, -33.0, 64.0)
            sx = (lanef + (b * 128).astype(f32)) + H * dx
            lx = jnp.clip(sx - (b * 128 - 64).astype(f32), -1.0, 256.0)
            base = jnp.floor(lx)
            frac = lx - base
            ix = base.astype(jnp.int32)
            w0 = jnp.where(ix < 0, frac, jnp.where(ix < 256, 1.0 - frac, 0.0)).astype(jnp.bfloat16).astype(f32)
            w1 = jnp.where((ix >= 0) & (ix < 255), frac, 0.0).astype(jnp.bfloat16).astype(f32)
            r = slice(8 * g, 8 * g + 8)
            low = jnp.floor(jnp.min(sy, axis=1, keepdims=True))
            rel = sy - low
            most = rel if most is None else jnp.maximum(most, rel)
            sp_s[b, r, :] = rel
            low_s[b, r, :] = jnp.broadcast_to(low, (8, 128))
            ix_s[b, r, :] = jnp.clip(ix, 0, 255)
            w0_s[b, r, :] = w0
            w1_s[b, r, :] = w1
        return jnp.where(lane == b, jnp.max(most, axis=1, keepdims=True), spans)

    spans = lax.fori_loop(0, blocks, prepare, jnp.zeros((8, 128), f32), unroll=UP)
    rows = jnp.floor(jnp.max(spans, axis=0, keepdims=True)).astype(jnp.int32) + 2
    extra = (jnp.maximum(rows - FIRST, 0) + (MORE - 1)) // MORE
    extra = jnp.where(lane[0:1] == blocks, jnp.max(extra, axis=1, keepdims=True), extra)
    num_v[...] = jnp.broadcast_to(extra, (8, 128))
    bring = pltpu.make_async_copy(num_v, num_m, sems.at[5])
    bring.start()

    own.wait()
    lanes = lax.broadcasted_iota(jnp.int32, (H, 128), 1)
    zero = jnp.zeros((H, 128), jnp.bfloat16)
    for at, rows_ref, there in ((0, wide_ref.at[0], tile > 0), (H, src_ref, None), (2 * H, wide_ref.at[1], tile < n - 1)):
        prev = [zero, zero]
        for k in range(blocks + 1):
            now = zero
            if k < blocks:
                now = rows_ref[:, 128 * k : 128 * k + 128]
                if there is not None:
                    now = jnp.where(there, now, zero)
            for p, (to, turn) in enumerate(((pages, 64), (pages1, 63))):
                turned = pltpu.roll(now, turn, 1) if k < blocks else zero
                to[at : at + H, 128 * k : 128 * k + 128] = jnp.where(lanes < turn, prev[p], turned)
                prev[p] = turned
    slot = lax.broadcasted_iota(jnp.int32, (8, 3 * H), 1)
    first = jnp.broadcast_to(first_ref[...].reshape(1, 1), slot.shape) * BH - tile * H + H
    last = first + jnp.broadcast_to(count_ref[...].reshape(1, 1), slot.shape) * BH
    slot = jnp.where((slot >= first) & (slot < last), (slot - H).astype(f32), -1e6)

    def source_of(b):
        cols = pl.ds(pl.multiple_of(b * 128, 128), 256)
        window = pages[:, cols], pages1[:, cols]
        lows = [low_s[b, 8 * g : 8 * g + 8, :][:, : 3 * H] for g in range(GROUPS)]
        return window, lows

    def pull(held, start, size):
        window, lows = held
        onehot = jnp.concatenate(
            [jnp.where(slot == lows[g] + (start + d), 1.0, 0.0) for g in range(GROUPS) for d in range(size)], axis=0)
        onehot = onehot.astype(jnp.bfloat16)
        return [jnp.dot(onehot, w, preferred_element_type=f32) for w in window]

    def blend(b, got, start, size, accs):
        out = []
        for g in range(GROUPS):
            r = slice(8 * g, 8 * g + 8)
            i0 = ix_s[b, r, :]
            rel = sp_s[b, r, :]
            ty = [jnp.maximum(0.0, 1.0 - jnp.abs(rel - (start + d))) for d in range(size)]
            acc = accs[g]
            here, m = i0 < 128, i0 & 127
            for tap, w_s in zip(got, (w0_s, w1_s)):
                total = None
                for d in range(size):
                    at = 8 * (g * size + d)
                    near, far = tap[at : at + 8, :128], tap[at : at + 8, 128:]
                    term = jnp.where(here, pick(near, m), pick(far, m)) * ty[d]
                    total = term if total is None else total + term
                total = total * w_s[b, r, :]
                acc = total if acc is None else acc + total
            out.append(acc)
        return tuple(out)

    def paint(q, _):
        bs = [q * UB + j for j in range(UB)]
        gots = [pull(source_of(b), 0.0, FIRST) for b in bs]
        for b, got in zip(bs, gots):
            accum[b] = jnp.concatenate(blend(b, got, 0.0, FIRST, (None,) * GROUPS), axis=0)
        return 0

    lax.fori_loop(0, blocks // UB, paint, 0)
    bring.wait()

    @pl.when(num_m[0, blocks] > 0)
    def _():
        def again(b, _):
            def more(k, accs):
                start = (FIRST + MORE * k).astype(f32)
                return blend(b, pull(source_of(b), start, MORE), start, MORE, accs)

            accs = lax.fori_loop(0, num_m[0, b], more, tuple(accum[b, 8 * g : 8 * g + 8, :] for g in range(GROUPS)))
            accum[b] = jnp.concatenate(accs, axis=0)
            return 0

        lax.fori_loop(0, blocks, again, 0)

    def emit(b, _):
        out_ref[:, pl.ds(pl.multiple_of(b * 128, 128), 128)] = accum[b].astype(jnp.bfloat16)
        return 0
    lax.fori_loop(0, blocks, emit, 0, unroll=4)


def render(first, count, fitted, source, wide):
    blocks = W // 128
    vm = pl.BlockSpec(memory_space=pltpu.VMEM)
    hbm = pl.BlockSpec(memory_space=pl.ANY)
    per = lambda d: pltpu.VMEM((blocks, H, 128), d)
    return pl.pallas_call(
        render_kernel,
        out_shape=(
            jax.ShapeDtypeStruct((H, W), jnp.bfloat16),
            jax.ShapeDtypeStruct((6, VR, VC), jnp.float32),
        ),
        in_specs=[vm, vm, vm, pl.BlockSpec(memory_space=pltpu.HBM), vm],
        out_specs=(vm, vm),
        scratch_shapes=[
            pltpu.VMEM((H, W), jnp.bfloat16),
            pltpu.VMEM((3 * H, W + 128), jnp.bfloat16),
            pltpu.VMEM((3 * H, W + 128), jnp.bfloat16),
            pltpu.VMEM((-(-blocks // PER), 16, 128), jnp.float32),
            per(jnp.float32), per(jnp.float32), per(jnp.int32), per(jnp.float32), per(jnp.float32), per(jnp.float32),
            pltpu.VMEM((8, 128), jnp.int32),
            pltpu.SMEM((8, 128), jnp.int32),
            pltpu.SemaphoreType.DMA((6,)),
        ],
        compiler_params=pltpu.CompilerParams(vmem_limit_bytes=16 << 20),
        name="render",
    )(first, count, fitted, source, wide)


def per_device(points, source, slab_first, slab_count):
    points, source = [pltpu.with_memory_space_constraint(x, pltpu.HBM) for x in (points, source)]
    fitted, wide = fit(points, source)
    rendered, affines = render(slab_first, slab_count, fitted, source, wide)
    return (rendered, affines)


def solution(mesh):
    return jax.shard_map(
        per_device,
        mesh=mesh,
        in_specs=(
            P(None, ("sec", "ty")),
            P(("sec", "ty"), None),
            P(("sec", "ty")),
            P(("sec", "ty")),
        ),
        out_specs=(P(("sec", "ty"), None), P(None, ("sec", "ty"), None)),
        check_vma=False,
    )
```

```python
import math

import jax
import jax.numpy as jnp
from jax import lax
from jax.experimental import pallas as pl
from jax.experimental.pallas import tpu as pltpu
from jax.sharding import PartitionSpec as P

W = 2048
BH = 16
SP = 8
H = 32
K = 6
VR = 4
VC = 256


MESH = pl.DeviceIdType.MESH
RIDGE_TERM = 0.01


def solve_affine(moments, vertex_x, vertex_y):
    scale = 1.0 / moments[0]
    mean_px, mean_py, mean_qx, mean_qy = [m * scale for m in moments[1:5]]
    cov_xx = moments[5] * scale - mean_px * mean_px + RIDGE_TERM
    cov_xy = moments[6] * scale - mean_px * mean_py
    cov_yy = moments[7] * scale - mean_py * mean_py + RIDGE_TERM
    cross_xx = moments[8] * scale - mean_qx * mean_px
    cross_xy = moments[9] * scale - mean_qx * mean_py
    cross_yx = moments[10] * scale - mean_qy * mean_px
    cross_yy = moments[11] * scale - mean_qy * mean_py
    inverse = 1.0 / (cov_xx * cov_yy - cov_xy * cov_xy)
    lin_xx = (cross_xx * cov_yy - cross_xy * cov_xy) * inverse
    lin_xy = (cross_xy * cov_xx - cross_xx * cov_xy) * inverse
    lin_yx = (cross_yx * cov_yy - cross_yy * cov_xy) * inverse
    lin_yy = (cross_yy * cov_xx - cross_yx * cov_xy) * inverse
    delta_x = vertex_x - mean_px
    delta_y = vertex_y - mean_py
    shift_x = mean_qx + lin_xx * delta_x + lin_xy * delta_y - vertex_x
    shift_y = mean_qy + lin_yx * delta_x + lin_yy * delta_y - vertex_y
    return [lin_xx, lin_xy, lin_yx, lin_yy, shift_x, shift_y]


OFFSETS = (1, -1, 2, -2)
FAR = 1e5
RATE = -2.0 * math.log2(math.e)
SKIP = 1e3


def halves(x):
    high = x.astype(jnp.bfloat16)
    return high, (x - high.astype(jnp.float32)).astype(jnp.bfloat16)


def fit_kernel(pts_ref, src_ref, fit_ref, wide,
               held, staged, mom, side, send_p, recv_p, send_s, recv_s, load):
    f32 = jnp.float32
    me = lax.axis_index("ty")
    n = lax.axis_size("ty")
    half = pts_ref.shape[1] // 2
    pairs = W // 256

    def exists(d):
        return (me + d >= 0) & (me + d < n)

    own_points = [
        pltpu.make_async_copy(pts_ref.at[:, pl.ds(c * half, half)], held.at[2, pl.ds(4 * c, 4)], load.at[c])
        for c in range(2)
    ]
    for c in own_points:
        c.start()
    barrier = pltpu.get_barrier_semaphore()
    for d in OFFSETS:
        @pl.when(exists(d))
        def _(d=d):
            pl.semaphore_signal(barrier, inc=1, device_id={"ty": me + d}, device_id_type=MESH)
    peers = sum(exists(d).astype(jnp.int32) for d in OFFSETS)

    def points_to(i, d):
        return pltpu.make_async_remote_copy(
            src_ref=held.at[2], dst_ref=held.at[2 - d], send_sem=send_p.at[i], recv_sem=recv_p.at[i],
            device_id={"ty": me + d}, device_id_type=MESH)

    def source_to(i, d):
        return pltpu.make_async_remote_copy(
            src_ref=src_ref, dst_ref=wide.at[i], send_sem=send_s.at[i], recv_sem=recv_s.at[i],
            device_id={"ty": me + d}, device_id_type=MESH)

    for c in own_points:
        c.wait()
    pl.semaphore_wait(barrier, peers)
    for i, d in enumerate(OFFSETS):
        @pl.when(exists(d))
        def _(i=i, d=d):
            points_to(i, d).start()
    for i, d in enumerate(OFFSETS[:2]):
        @pl.when(exists(d))
        def _(i=i, d=d):
            source_to(i, d).start()

    wide_lane = lax.broadcasted_iota(jnp.int32, (8, half + 128), 1) // 128
    wide_row = lax.broadcasted_iota(jnp.int32, (8, half + 128), 0) % 2
    centre = (me * H).astype(f32) + H / 2.0
    anchors = [
        jnp.where(wide_row == 0, ((2 * wide_lane + odd) * 256 + 128).astype(f32), centre) * (1.0 / H)
        for odd in range(2)
    ]
    spare = jnp.full((8, 128), FAR, f32)

    def stage(tile):
        data = held[2] if tile == 2 else jnp.where(exists(tile - 2), held[tile], FAR)
        row = jnp.concatenate([data, spare], axis=1) * (1.0 / H)
        staged[0, tile] = pltpu.roll(row, 32, 1) - anchors[0]
        staged[1, tile] = pltpu.roll(row, half + 96, 1) - anchors[1]

    e = lax.broadcasted_iota(jnp.int32, (8, 128), 0)
    vy = (((e - 1) * SP + SP // 2) - H // 2).astype(f32) * (1.0 / H)
    vy_of = {1: jnp.where(e == 5, SKIP, vy), 2: vy, 3: jnp.where(e == 0, SKIP, vy)}
    lone = {0: (-SP // 2 - H // 2) / H, 4: (4 * SP + SP // 2 - H // 2) / H}
    lane32 = lax.broadcasted_iota(jnp.int32, (32, 128), 1)
    vert32 = lax.broadcasted_iota(jnp.int32, (32, 128), 0)
    near = jnp.abs(lane32 // 32 - 1 - vert32 // 16) <= 1
    vx = jnp.where(near, (vert32 * SP + SP // 2 - 128).astype(f32) * (1.0 / H), SKIP)

    def bell(gap):
        return jnp.exp2((gap * gap) * RATE)

    def rows_of(k, odd, tile, c):
        at = pl.ds(pl.multiple_of(k * 128, 128), 128)
        return [jnp.broadcast_to(staged[odd, tile, 4 * c + i : 4 * c + i + 1, at], (8, 128)) for i in range(4)]

    def across(px):
        gap = jnp.concatenate([px - vx[8 * g : 8 * g + 8] for g in range(4)], axis=0)
        return jnp.concatenate(halves(bell(gap)), axis=0)

    def contract(parts, weights):
        return lax.dot_general(
            jnp.concatenate(parts, axis=1), jnp.concatenate(weights, axis=1),
            (((1,), (1,)), ((), ())), preferred_element_type=f32)

    def dense(k, odd, tiles):
        parts, weights = [], []
        for tile in tiles:
            for c in range(2):
                px, py, qx, qy = rows_of(k, odd, tile, c)
                weights.append(across(px))
                w = bell(py - vy_of[tile])
                wpx = w * px
                wpy = w * py
                feats = jnp.concatenate(
                    [w, wpx, wpy, w * qx, w * qy, wpx * px, wpx * py, wpy * py,
                     wpx * qx, wpy * qx, wpx * qy, wpy * qy], axis=0)
                parts.append(jnp.concatenate(halves(feats), axis=0))
        got = contract(parts, weights)
        got = got[0:96] + got[96:192]
        return got[:, 0:32] + got[:, 32:64]

    def single(k, odd, tile):
        parts, weights = [], []
        for c in range(2):
            px, py, qx, qy = rows_of(k, odd, tile, c)
            weights.append(across(px))
            w = bell(py - lone[tile])
            a1 = jnp.where(e == 0, 1.0, jnp.where((e == 2) | (e == 7), py, jnp.where(e == 3, qx, jnp.where(e == 4, qy, px))))
            b1 = jnp.where(e < 5, 1.0, jnp.where(e == 5, px, py))
            a2 = jnp.where(e % 2 == 0, px, py)
            b2 = jnp.where(e < 2, qx, qy)
            feats = jnp.concatenate([w * a1 * b1, w * a2 * b2], axis=0)
            parts.append(jnp.concatenate(halves(feats), axis=0))
        got = contract(parts, weights)
        got = got[0:16] + got[16:32]
        return got[:, 0:32] + got[:, 32:64]

    def own_group(k, _):
        for odd in range(2):
            mom[2 * k + odd] = dense(k, odd, (2,))
        return 0

    def next_group(k, _):
        for odd in range(2):
            mom[2 * k + odd] += dense(k, odd, (1, 3))
        return 0

    def last_group(k, _):
        for odd in range(2):
            for s, tile in enumerate((0, 4)):
                side[s, 2 * k + odd] = single(k, odd, tile)
        return 0

    def arrive(which):
        for i in which:
            @pl.when(exists(-OFFSETS[i]))
            def _(i=i):
                points_to(i, OFFSETS[i]).wait_recv()
        for i in which:
            stage(2 - OFFSETS[i])

    stage(2)
    lax.fori_loop(0, pairs // 2, own_group, 0, unroll=4)
    arrive((0, 1))
    lax.fori_loop(0, pairs // 2, next_group, 0, unroll=4)
    arrive((2, 3))
    lax.fori_loop(0, pairs // 2, last_group, 0, unroll=4)

    ew = lax.broadcasted_iota(jnp.int32, (8, VC), 0)
    jw = lax.broadcasted_iota(jnp.int32, (8, VC), 1)
    vertex_y = (((ew - 1) * SP + SP // 2) - H // 2).astype(f32) * (1.0 / H)
    vertex_x = ((jw % 32) * SP + SP // 2 - 128).astype(f32) * (1.0 / H)
    safe = ew < 6
    sides = [jnp.concatenate([side[s, g] for g in range(pairs)], axis=1) for s in range(2)]
    moments = []
    for f in range(12):
        m = jnp.concatenate([mom[g, 8 * f : 8 * f + 8, :] for g in range(pairs)], axis=1)
        m = m + jnp.where(ew == 0, sides[0][f : f + 1], jnp.where(ew == 5, sides[1][f : f + 1], 0.0))
        moments.append(m)
    moments[0] = jnp.where(safe, moments[0], 1.0)
    solved = solve_affine(moments, vertex_x, vertex_y)
    for f in range(6):
        x = solved[f]
        if f >= 4:
            x = jnp.where((ew == 0) & (me == 0), x[1:2], x)
            x = jnp.where((ew == 5) & (me == n - 1), x[4:5], x)
            x = jnp.where(safe, x, 0.0)
        fit_ref[8 * f : 8 * f + 8, :] = x

    for i, d in enumerate(OFFSETS[:2]):
        @pl.when(exists(-d))
        def _(i=i, d=d):
            source_to(i, d).wait_recv()
    for i, d in enumerate(OFFSETS):
        @pl.when(exists(d))
        def _(i=i, d=d):
            points_to(i, d).wait_send()
    for i, d in enumerate(OFFSETS[:2]):
        @pl.when(exists(d))
        def _(i=i, d=d):
            source_to(i, d).wait_send()


def fit(points, source):
    size = points.shape[1]
    vm = pl.BlockSpec(memory_space=pltpu.VMEM)
    return pl.pallas_call(
        fit_kernel,
        out_shape=(
            pltpu.VMEM((48, VC), jnp.float32),
            pltpu.VMEM((2, H, W), jnp.bfloat16),
        ),
        in_specs=[pl.BlockSpec(memory_space=pltpu.HBM)] * 2,
        out_specs=(vm, vm),
        scratch_shapes=[
            pltpu.VMEM((5, 8, size // 2), jnp.float32),
            pltpu.VMEM((2, 5, 8, size // 2 + 128), jnp.float32),
            pltpu.VMEM((W // 256, 96, 32), jnp.float32),
            pltpu.VMEM((2, W // 256, 16, 32), jnp.float32),
            pltpu.SemaphoreType.DMA((4,)),
            pltpu.SemaphoreType.DMA((4,)),
            pltpu.SemaphoreType.DMA((2,)),
            pltpu.SemaphoreType.DMA((2,)),
            pltpu.SemaphoreType.DMA((2,)),
        ],
        compiler_params=pltpu.CompilerParams(collective_id=0, has_side_effects=True, vmem_limit_bytes=8 << 20),
        name="fit",
    )(points, source)


GROUPS = H // SP
FIRST = 8
UB = 16
UP = 4
MORE = 2
PER = 7


def pick(x, lanes):
    dims = lax.GatherDimensionNumbers(
        offset_dims=(), collapsed_slice_dims=(1,), start_index_map=(1,),
        operand_batching_dims=(0,), start_indices_batching_dims=(0,))
    return lax.gather(x, lanes[..., None], dims, slice_sizes=(1, 1),
                      mode=lax.GatherScatterMode.PROMISE_IN_BOUNDS)


def render_kernel(first_ref, count_ref, fit_ref, own_ref, wide_ref, out_ref, aff_ref,
                  src_ref, pages, pages1, ext, sp_s, low_s, far_s, ix_s, w0_s, w1_s, accum, num_v, num_m, sems):
    blocks = W // 128
    tile = lax.axis_index("ty")
    n = lax.axis_size("ty")
    f32 = jnp.float32
    own = pltpu.make_async_copy(own_ref, src_ref, sems.at[2])
    own.start()
    for f in range(6):
        aff_ref[f] = fit_ref[8 * f + 1 : 8 * f + 5, :]

    left, right = fit_ref[32:48, 0:128], fit_ref[32:48, 128:256]
    lane16 = lax.broadcasted_iota(jnp.int32, (16, 128), 1)
    ext[0] = jnp.where(lane16 < 1, left[:, 0:1], pltpu.roll(left, 1, 1))
    ext[1] = jnp.where(lane16 < 17, pltpu.roll(left, 17, 1), pltpu.roll(right, 17, 1))
    ext[2] = jnp.where(lane16 < 33, pltpu.roll(right, 33, 1), right[:, 127:128])

    sub = lax.broadcasted_iota(jnp.int32, (8, 128), 0)
    subf = sub.astype(f32)
    lane = lax.broadcasted_iota(jnp.int32, (8, 128), 1)
    wa = jnp.maximum(0.0, 1.0 - (subf + 4.0) * (1.0 / SP))
    wb = jnp.maximum(0.0, 1.0 - jnp.abs(subf - 4.0) * (1.0 / SP))
    wc = jnp.maximum(0.0, 1.0 - (12.0 - subf) * (1.0 / SP))
    lanef = lane.astype(f32)
    step = (lane + SP // 2) // SP
    part = ((lane + SP // 2) % SP).astype(f32) * (1.0 / SP)

    def prepare(b, spans):
        page = b // PER
        at = step + (b - page * PER) * (128 // SP)
        fine = []
        for half in range(2):
            held = ext[page, 8 * half : 8 * half + 8, :]
            near = pick(held, at)
            fine.append(near + part * (pick(held, at + 1) - near))
        fx, fy = fine
        most = None
        for g in range(GROUPS):
            dx = wa * fx[g : g + 1] + wb * fx[g + 1 : g + 2] + wc * fx[g + 2 : g + 3]
            dy = wa * fy[g : g + 1] + wb * fy[g + 1 : g + 2] + wc * fy[g + 2 : g + 3]
            sy = jnp.clip(subf + (8.0 * g) + H * dy, -33.0, 64.0)
            sx = (lanef + (b * 128).astype(f32)) + H * dx
            lx = jnp.clip(sx - (b * 128 - 64).astype(f32), -1.0, 256.0)
            base = jnp.floor(lx)
            frac = lx - base
            ix = base.astype(jnp.int32)
            w0 = jnp.where(ix < 0, frac, jnp.where(ix < 256, 1.0 - frac, 0.0)).astype(jnp.bfloat16).astype(f32)
            w1 = jnp.where((ix >= 0) & (ix < 255), frac, 0.0).astype(jnp.bfloat16).astype(f32)
            r = slice(8 * g, 8 * g + 8)
            low = jnp.floor(jnp.min(sy, axis=1, keepdims=True))
            rel = sy - low
            most = rel if most is None else jnp.maximum(most, rel)
            sp_s[b, r, :] = rel
            low_s[b, r, :] = jnp.broadcast_to(low, (8, 128))
            ix = jnp.clip(ix, 0, 255)
            far_s[b, r, :] = jnp.where(ix < 128, 0.0, 1.0)
            ix_s[b, 16 * g : 16 * g + 16, :] = jnp.concatenate([ix, ix], axis=0).astype(jnp.int16)
            w0_s[b, r, :] = w0
            w1_s[b, r, :] = w1
        return jnp.where(lane == b, jnp.max(most, axis=1, keepdims=True), spans)

    spans = lax.fori_loop(0, blocks, prepare, jnp.zeros((8, 128), f32), unroll=UP)
    rows = jnp.floor(jnp.max(spans, axis=0, keepdims=True)).astype(jnp.int32) + 2
    extra = (jnp.maximum(rows - FIRST, 0) + (MORE - 1)) // MORE
    extra = jnp.where(lane[0:1] == blocks, jnp.max(extra, axis=1, keepdims=True), extra)
    num_v[...] = jnp.broadcast_to(extra, (8, 128))
    bring = pltpu.make_async_copy(num_v, num_m, sems.at[5])
    bring.start()

    own.wait()
    lanes = lax.broadcasted_iota(jnp.int32, (H, 128), 1)
    zero = jnp.zeros((H, 128), jnp.bfloat16)
    for at, rows_ref, there in ((0, wide_ref.at[0], tile > 0), (H, src_ref, None), (2 * H, wide_ref.at[1], tile < n - 1)):
        prev = [zero, zero]
        for k in range(blocks + 1):
            now = zero
            if k < blocks:
                now = rows_ref[:, 128 * k : 128 * k + 128]
                if there is not None:
                    now = jnp.where(there, now, zero)
            for p, (to, turn) in enumerate(((pages, 64), (pages1, 63))):
                turned = pltpu.roll(now, turn, 1) if k < blocks else zero
                to[at : at + H, 128 * k : 128 * k + 128] = jnp.where(lanes < turn, prev[p], turned)
                prev[p] = turned
    slot = lax.broadcasted_iota(jnp.int32, (8, 3 * H), 1)
    first = jnp.broadcast_to(first_ref[...].reshape(1, 1), slot.shape) * BH - tile * H + H
    last = first + jnp.broadcast_to(count_ref[...].reshape(1, 1), slot.shape) * BH
    slot = jnp.where((slot >= first) & (slot < last), (slot - H).astype(f32), -1e6)

    def source_of(b):
        cols = pl.ds(pl.multiple_of(b * 128, 128), 256)
        window = pages[:, cols], pages1[:, cols]
        lows = [low_s[b, 8 * g : 8 * g + 8, :][:, : 3 * H] for g in range(GROUPS)]
        return window, lows

    def pull(held, start, size):
        window, lows = held
        onehot = jnp.concatenate(
            [jnp.where(slot == lows[g] + (start + d), 1.0, 0.0) for g in range(GROUPS) for d in range(size)], axis=0)
        onehot = onehot.astype(jnp.bfloat16)
        return [jnp.dot(onehot, w, preferred_element_type=f32) for w in window]

    def blend(b, got, start, size, accs):
        out = []
        for g in range(GROUPS):
            r = slice(8 * g, 8 * g + 8)
            lanes_at = ix_s[b, 16 * g : 16 * g + 16, :]
            m = lanes_at & 127
            here = far_s[b, r, :] < 0.5
            rel = sp_s[b, r, :]
            totals = [None, None]
            for d in range(size):
                at = slice(8 * (g * size + d), 8 * (g * size + d) + 8)
                near, far = [
                    jnp.concatenate([tap[at, side] for tap in got], axis=0).astype(jnp.bfloat16)
                    for side in (slice(0, 128), slice(128, 256))
                ]
                near, far = pick(near, m).astype(f32), pick(far, m).astype(f32)
                ty = jnp.maximum(0.0, 1.0 - jnp.abs(rel - (start + d)))
                for p in range(2):
                    term = jnp.where(here, near[8 * p : 8 * p + 8], far[8 * p : 8 * p + 8]) * ty
                    totals[p] = term if d == 0 else totals[p] + term
            res = totals[0] * w0_s[b, r, :] + totals[1] * w1_s[b, r, :]
            out.append(res if accs[g] is None else accs[g] + res)
        return tuple(out)

    def paint(q, _):
        bs = [q * UB + j for j in range(UB)]
        gots = [pull(source_of(b), 0.0, FIRST) for b in bs]
        for b, got in zip(bs, gots):
            accum[b] = jnp.concatenate(blend(b, got, 0.0, FIRST, (None,) * GROUPS), axis=0)
        return 0

    lax.fori_loop(0, blocks // UB, paint, 0)
    bring.wait()

    @pl.when(num_m[0, blocks] > 0)
    def _():
        def again(b, _):
            def more(k, accs):
                start = (FIRST + MORE * k).astype(f32)
                return blend(b, pull(source_of(b), start, MORE), start, MORE, accs)

            accs = lax.fori_loop(0, num_m[0, b], more, tuple(accum[b, 8 * g : 8 * g + 8, :] for g in range(GROUPS)))
            accum[b] = jnp.concatenate(accs, axis=0)
            return 0

        lax.fori_loop(0, blocks, again, 0)

    def emit(b, _):
        out_ref[:, pl.ds(pl.multiple_of(b * 128, 128), 128)] = accum[b].astype(jnp.bfloat16)
        return 0
    lax.fori_loop(0, blocks, emit, 0, unroll=4)


def render(first, count, fitted, source, wide):
    blocks = W // 128
    vm = pl.BlockSpec(memory_space=pltpu.VMEM)
    hbm = pl.BlockSpec(memory_space=pl.ANY)
    per = lambda d: pltpu.VMEM((blocks, H, 128), d)
    return pl.pallas_call(
        render_kernel,
        out_shape=(
            jax.ShapeDtypeStruct((H, W), jnp.bfloat16),
            jax.ShapeDtypeStruct((6, VR, VC), jnp.float32),
        ),
        in_specs=[vm, vm, vm, pl.BlockSpec(memory_space=pltpu.HBM), vm],
        out_specs=(vm, vm),
        scratch_shapes=[
            pltpu.VMEM((H, W), jnp.bfloat16),
            pltpu.VMEM((3 * H, W + 128), jnp.bfloat16),
            pltpu.VMEM((3 * H, W + 128), jnp.bfloat16),
            pltpu.VMEM((-(-blocks // PER), 16, 128), jnp.float32),
            per(jnp.float32), per(jnp.float32), per(jnp.float32), pltpu.VMEM((blocks, 2 * H, 128), jnp.int16), per(jnp.float32), per(jnp.float32), per(jnp.float32),
            pltpu.VMEM((8, 128), jnp.int32),
            pltpu.SMEM((8, 128), jnp.int32),
            pltpu.SemaphoreType.DMA((6,)),
        ],
        compiler_params=pltpu.CompilerParams(vmem_limit_bytes=16 << 20),
        name="render",
    )(first, count, fitted, source, wide)


def per_device(points, source, slab_first, slab_count):
    points, source = [pltpu.with_memory_space_constraint(x, pltpu.HBM) for x in (points, source)]
    fitted, wide = fit(points, source)
    rendered, affines = render(slab_first, slab_count, fitted, source, wide)
    return (rendered, affines)


def solution(mesh):
    return jax.shard_map(
        per_device,
        mesh=mesh,
        in_specs=(
            P(None, ("sec", "ty")),
            P(("sec", "ty"), None),
            P(("sec", "ty")),
            P(("sec", "ty")),
        ),
        out_specs=(P(("sec", "ty"), None), P(None, ("sec", "ty"), None)),
        check_vma=False,
    )
```

```python
import math

import jax
import jax.numpy as jnp
from jax import lax
from jax.experimental import pallas as pl
from jax.experimental.pallas import tpu as pltpu
from jax.sharding import PartitionSpec as P

W = 2048
BH = 16
SP = 8
H = 32
K = 6
VR = 4
VC = 256


MESH = pl.DeviceIdType.MESH
RIDGE_TERM = 0.01


def solve_affine(moments, vertex_x, vertex_y):
    scale = 1.0 / moments[0]
    mean_px, mean_py, mean_qx, mean_qy = [m * scale for m in moments[1:5]]
    cov_xx = moments[5] * scale - mean_px * mean_px + RIDGE_TERM
    cov_xy = moments[6] * scale - mean_px * mean_py
    cov_yy = moments[7] * scale - mean_py * mean_py + RIDGE_TERM
    cross_xx = moments[8] * scale - mean_qx * mean_px
    cross_xy = moments[9] * scale - mean_qx * mean_py
    cross_yx = moments[10] * scale - mean_qy * mean_px
    cross_yy = moments[11] * scale - mean_qy * mean_py
    inverse = 1.0 / (cov_xx * cov_yy - cov_xy * cov_xy)
    lin_xx = (cross_xx * cov_yy - cross_xy * cov_xy) * inverse
    lin_xy = (cross_xy * cov_xx - cross_xx * cov_xy) * inverse
    lin_yx = (cross_yx * cov_yy - cross_yy * cov_xy) * inverse
    lin_yy = (cross_yy * cov_xx - cross_yx * cov_xy) * inverse
    delta_x = vertex_x - mean_px
    delta_y = vertex_y - mean_py
    shift_x = mean_qx + lin_xx * delta_x + lin_xy * delta_y - vertex_x
    shift_y = mean_qy + lin_yx * delta_x + lin_yy * delta_y - vertex_y
    return [lin_xx, lin_xy, lin_yx, lin_yy, shift_x, shift_y]


GROUPS = H // SP
FIRST = 8
UB = 16
UP = 4
MORE = 2
PER = 7


def pick(x, lanes):
    dims = lax.GatherDimensionNumbers(
        offset_dims=(), collapsed_slice_dims=(1,), start_index_map=(1,),
        operand_batching_dims=(0,), start_indices_batching_dims=(0,))
    return lax.gather(x, lanes[..., None], dims, slice_sizes=(1, 1),
                      mode=lax.GatherScatterMode.PROMISE_IN_BOUNDS)


def page_rows(rows_ref, to, there):
    lanes = lax.broadcasted_iota(jnp.int32, (H, 128), 1)
    zero = jnp.zeros((H, 128), jnp.bfloat16)
    prev = [zero, zero]
    for k in range(W // 128 + 1):
        now = zero
        if k < W // 128:
            now = rows_ref[:, 128 * k : 128 * k + 128]
            if there is not None:
                now = jnp.where(there, now, zero)
        for p, turn in enumerate((64, 63)):
            turned = pltpu.roll(now, turn, 1) if k < W // 128 else zero
            to[p, :, 128 * k : 128 * k + 128] = jnp.where(lanes < turn, prev[p], turned)
            prev[p] = turned


def positions(shifts, ext, num_ref, sp_s, low_s, far_s, ix_s, w0_s, w1_s):
    blocks = W // 128
    f32 = jnp.float32
    left, right = shifts[:, 0:128], shifts[:, 128:256]
    lane16 = lax.broadcasted_iota(jnp.int32, (16, 128), 1)
    ext[0] = jnp.where(lane16 < 1, left[:, 0:1], pltpu.roll(left, 1, 1))
    ext[1] = jnp.where(lane16 < 17, pltpu.roll(left, 17, 1), pltpu.roll(right, 17, 1))
    ext[2] = jnp.where(lane16 < 33, pltpu.roll(right, 33, 1), right[:, 127:128])

    sub = lax.broadcasted_iota(jnp.int32, (8, 128), 0)
    subf = sub.astype(f32)
    lane = lax.broadcasted_iota(jnp.int32, (8, 128), 1)
    wa = jnp.maximum(0.0, 1.0 - (subf + 4.0) * (1.0 / SP))
    wb = jnp.maximum(0.0, 1.0 - jnp.abs(subf - 4.0) * (1.0 / SP))
    wc = jnp.maximum(0.0, 1.0 - (12.0 - subf) * (1.0 / SP))
    wa, wb, wc = H * wa, H * wb, H * wc
    column = lane.astype(f32) + 64.0
    step = (lane + SP // 2) // SP
    part = ((lane + SP // 2) % SP).astype(f32) * (1.0 / SP)

    def prepare(b, spans):
        page = b // PER
        at = step + (b - page * PER) * (128 // SP)
        fine = []
        for half in range(2):
            held = ext[page, 8 * half : 8 * half + 8, :]
            near = pick(held, at)
            fine.append(near + part * (pick(held, at + 1) - near))
        fx, fy = fine
        most = None
        for g in range(GROUPS):
            dx = wa * fx[g : g + 1] + wb * fx[g + 1 : g + 2] + wc * fx[g + 2 : g + 3]
            dy = wa * fy[g : g + 1] + wb * fy[g + 1 : g + 2] + wc * fy[g + 2 : g + 3]
            sy = jnp.clip((subf + 8.0 * g) + dy, -33.0, 64.0)
            lx = jnp.clip(column + dx, -1.0, 256.0)
            base = jnp.clip(jnp.floor(lx), 0.0, 255.0)
            past = lx - base
            taps = [1.0 - jnp.abs(past), jnp.maximum(jnp.minimum(past, 255.0 - base), 0.0)]
            low = jnp.floor(jnp.min(sy, axis=1, keepdims=True))
            rel = sy - low
            most = rel if most is None else jnp.maximum(most, rel)
            r, tall = slice(8 * g, 8 * g + 8), slice(16 * g, 16 * g + 16)
            sp_s[b, r, :] = rel
            low_s[b, r, :] = jnp.broadcast_to(low, (8, 128))
            far_s[b, r, :] = base
            at = base.astype(jnp.int32)
            ix_s[b, tall, :] = jnp.concatenate([at, at], axis=0).astype(jnp.int16)
            taps = jnp.concatenate(taps, axis=0).astype(jnp.bfloat16).astype(f32)
            w0_s[b, r, :] = taps[0:8]
            w1_s[b, r, :] = taps[8:16]
        return jnp.where(lane == b, jnp.max(most, axis=1, keepdims=True), spans)

    spans = jnp.zeros((8, 128), f32)
    for b in range(blocks):
        spans = prepare(b, spans)
    rows = jnp.floor(jnp.max(spans, axis=0, keepdims=True)).astype(jnp.int32) + 2
    extra = (jnp.maximum(rows - FIRST, 0) + (MORE - 1)) // MORE
    extra = jnp.where(lane[0:1] == blocks, jnp.max(extra, axis=1, keepdims=True), extra)
    num_ref[...] = jnp.broadcast_to(extra, (8, 128))


OFFSETS = (1, -1, 2, -2)
FAR = 1e5
RATE = -2.0 * math.log2(math.e)
SKIP = 1e3


def halves(x):
    high = x.astype(jnp.bfloat16)
    return high, (x - high.astype(jnp.float32)).astype(jnp.bfloat16)


def fit_kernel(pts_ref, src_ref, fit_ref, num_ref, sp_s, low_s, far_s, ix_s, w0_s, w1_s, paged, wide,
               rows_s, ext, held, staged, mom, side, send_p, recv_p, send_s, recv_s, load):
    f32 = jnp.float32
    me = lax.axis_index("ty")
    n = lax.axis_size("ty")
    half = pts_ref.shape[1] // 2
    pairs = W // 256

    def exists(d):
        return (me + d >= 0) & (me + d < n)

    own_points = [
        pltpu.make_async_copy(pts_ref.at[:, pl.ds(c * half, half)], held.at[2, pl.ds(4 * c, 4)], load.at[c])
        for c in range(2)
    ]
    for c in own_points:
        c.start()
    own_rows = pltpu.make_async_copy(src_ref, rows_s, load.at[2])
    own_rows.start()
    barrier = pltpu.get_barrier_semaphore()
    for d in OFFSETS:
        @pl.when(exists(d))
        def _(d=d):
            pl.semaphore_signal(barrier, inc=1, device_id={"ty": me + d}, device_id_type=MESH)
    peers = sum(exists(d).astype(jnp.int32) for d in OFFSETS)

    def points_to(i, d):
        return pltpu.make_async_remote_copy(
            src_ref=held.at[2], dst_ref=held.at[2 - d], send_sem=send_p.at[i], recv_sem=recv_p.at[i],
            device_id={"ty": me + d}, device_id_type=MESH)

    def source_to(i, d):
        return pltpu.make_async_remote_copy(
            src_ref=src_ref, dst_ref=wide.at[i], send_sem=send_s.at[i], recv_sem=recv_s.at[i],
            device_id={"ty": me + d}, device_id_type=MESH)

    for c in own_points:
        c.wait()
    pl.semaphore_wait(barrier, peers)
    for i, d in enumerate(OFFSETS):
        @pl.when(exists(d))
        def _(i=i, d=d):
            points_to(i, d).start()
    for i, d in enumerate(OFFSETS[:2]):
        @pl.when(exists(d))
        def _(i=i, d=d):
            source_to(i, d).start()

    wide_lane = lax.broadcasted_iota(jnp.int32, (8, half + 128), 1) // 128
    wide_row = lax.broadcasted_iota(jnp.int32, (8, half + 128), 0) % 2
    centre = (me * H).astype(f32) + H / 2.0
    anchors = [
        jnp.where(wide_row == 0, ((2 * wide_lane + odd) * 256 + 128).astype(f32), centre) * (1.0 / H)
        for odd in range(2)
    ]
    spare = jnp.full((8, 128), FAR, f32)

    def stage(tile):
        data = held[2] if tile == 2 else jnp.where(exists(tile - 2), held[tile], FAR)
        row = jnp.concatenate([data, spare], axis=1) * (1.0 / H)
        staged[0, tile] = pltpu.roll(row, 32, 1) - anchors[0]
        staged[1, tile] = pltpu.roll(row, half + 96, 1) - anchors[1]

    e = lax.broadcasted_iota(jnp.int32, (8, 128), 0)
    vy = (((e - 1) * SP + SP // 2) - H // 2).astype(f32) * (1.0 / H)
    vy_of = {1: jnp.where(e == 5, SKIP, vy), 2: vy, 3: jnp.where(e == 0, SKIP, vy)}
    lone = {0: (-SP // 2 - H // 2) / H, 4: (4 * SP + SP // 2 - H // 2) / H}
    lane32 = lax.broadcasted_iota(jnp.int32, (32, 128), 1)
    vert32 = lax.broadcasted_iota(jnp.int32, (32, 128), 0)
    near = jnp.abs(lane32 // 32 - 1 - vert32 // 16) <= 1
    vx = jnp.where(near, (vert32 * SP + SP // 2 - 128).astype(f32) * (1.0 / H), SKIP)

    def bell(gap):
        return jnp.exp2((gap * gap) * RATE)

    def rows_of(k, odd, tile, c):
        at = pl.ds(pl.multiple_of(k * 128, 128), 128)
        return [jnp.broadcast_to(staged[odd, tile, 4 * c + i : 4 * c + i + 1, at], (8, 128)) for i in range(4)]

    def across(px):
        gap = jnp.concatenate([px - vx[8 * g : 8 * g + 8] for g in range(4)], axis=0)
        return jnp.concatenate(halves(bell(gap)), axis=0)

    def contract(parts, weights):
        return lax.dot_general(
            jnp.concatenate(parts, axis=1), jnp.concatenate(weights, axis=1),
            (((1,), (1,)), ((), ())), preferred_element_type=f32)

    def dense(k, odd, tiles):
        parts, weights = [], []
        for tile in tiles:
            for c in range(2):
                px, py, qx, qy = rows_of(k, odd, tile, c)
                weights.append(across(px))
                w = bell(py - vy_of[tile])
                wpx = w * px
                wpy = w * py
                feats = jnp.concatenate(
                    [w, wpx, wpy, w * qx, w * qy, wpx * px, wpx * py, wpy * py,
                     wpx * qx, wpy * qx, wpx * qy, wpy * qy], axis=0)
                parts.append(jnp.concatenate(halves(feats), axis=0))
        got = contract(parts, weights)
        got = got[0:96] + got[96:192]
        return got[:, 0:32] + got[:, 32:64]

    def single(k, odd, tile):
        parts, weights = [], []
        for c in range(2):
            px, py, qx, qy = rows_of(k, odd, tile, c)
            weights.append(across(px))
            w = bell(py - lone[tile])
            a1 = jnp.where(e == 0, 1.0, jnp.where((e == 2) | (e == 7), py, jnp.where(e == 3, qx, jnp.where(e == 4, qy, px))))
            b1 = jnp.where(e < 5, 1.0, jnp.where(e == 5, px, py))
            a2 = jnp.where(e % 2 == 0, px, py)
            b2 = jnp.where(e < 2, qx, qy)
            feats = jnp.concatenate([w * a1 * b1, w * a2 * b2], axis=0)
            parts.append(jnp.concatenate(halves(feats), axis=0))
        got = contract(parts, weights)
        got = got[0:16] + got[16:32]
        return got[:, 0:32] + got[:, 32:64]

    def own_group(k, _):
        for odd in range(2):
            mom[2 * k + odd] = dense(k, odd, (2,))
        return 0

    def next_group(k, _):
        for odd in range(2):
            mom[2 * k + odd] += dense(k, odd, (1, 3))
        return 0

    def last_group(k, _):
        for odd in range(2):
            for s, tile in enumerate((0, 4)):
                side[s, 2 * k + odd] = single(k, odd, tile)
        return 0

    def arrive(which):
        for i in which:
            @pl.when(exists(-OFFSETS[i]))
            def _(i=i):
                points_to(i, OFFSETS[i]).wait_recv()
        for i in which:
            stage(2 - OFFSETS[i])

    stage(2)
    lax.fori_loop(0, pairs // 2, own_group, 0, unroll=4)
    own_rows.wait()
    page_rows(rows_s, paged, None)
    arrive((0, 1))
    lax.fori_loop(0, pairs // 2, next_group, 0, unroll=4)
    arrive((2, 3))
    lax.fori_loop(0, pairs // 2, last_group, 0, unroll=4)

    ew = lax.broadcasted_iota(jnp.int32, (8, VC), 0)
    jw = lax.broadcasted_iota(jnp.int32, (8, VC), 1)
    vertex_y = (((ew - 1) * SP + SP // 2) - H // 2).astype(f32) * (1.0 / H)
    vertex_x = ((jw % 32) * SP + SP // 2 - 128).astype(f32) * (1.0 / H)
    safe = ew < 6
    sides = [jnp.concatenate([side[s, g] for g in range(pairs)], axis=1) for s in range(2)]
    moments = []
    for f in range(12):
        m = jnp.concatenate([mom[g, 8 * f : 8 * f + 8, :] for g in range(pairs)], axis=1)
        m = m + jnp.where(ew == 0, sides[0][f : f + 1], jnp.where(ew == 5, sides[1][f : f + 1], 0.0))
        moments.append(m)
    moments[0] = jnp.where(safe, moments[0], 1.0)
    solved = solve_affine(moments, vertex_x, vertex_y)
    for f in range(6):
        x = solved[f]
        if f >= 4:
            x = jnp.where((ew == 0) & (me == 0), x[1:2], x)
            x = jnp.where((ew == 5) & (me == n - 1), x[4:5], x)
            x = jnp.where(safe, x, 0.0)
        fit_ref[8 * f : 8 * f + 8, :] = x
        solved[f] = x
    positions(jnp.concatenate(solved[4:6], axis=0), ext, num_ref, sp_s, low_s, far_s, ix_s, w0_s, w1_s)

    for i, d in enumerate(OFFSETS[:2]):
        @pl.when(exists(-d))
        def _(i=i, d=d):
            source_to(i, d).wait_recv()
    for i, d in enumerate(OFFSETS):
        @pl.when(exists(d))
        def _(i=i, d=d):
            points_to(i, d).wait_send()
    for i, d in enumerate(OFFSETS[:2]):
        @pl.when(exists(d))
        def _(i=i, d=d):
            source_to(i, d).wait_send()


def fit(points, source):
    size = points.shape[1]
    blocks = W // 128
    per = lambda d: pltpu.VMEM((blocks, H, 128), d)
    vm = pl.BlockSpec(memory_space=pltpu.VMEM)
    return pl.pallas_call(
        fit_kernel,
        out_shape=(
            pltpu.VMEM((48, VC), jnp.float32),
            pltpu.VMEM((8, 128), jnp.int32),
            per(jnp.float32), per(jnp.float32), per(jnp.float32),
            pltpu.VMEM((blocks, 2 * H, 128), jnp.int16),
            per(jnp.float32), per(jnp.float32),
            pltpu.VMEM((2, H, W + 128), jnp.bfloat16),
            pltpu.VMEM((2, H, W), jnp.bfloat16),
        ),
        in_specs=[pl.BlockSpec(memory_space=pltpu.HBM)] * 2,
        out_specs=(vm,) * 10,
        scratch_shapes=[
            pltpu.VMEM((H, W), jnp.bfloat16),
            pltpu.VMEM((-(-blocks // PER), 16, 128), jnp.float32),
            pltpu.VMEM((5, 8, size // 2), jnp.float32),
            pltpu.VMEM((2, 5, 8, size // 2 + 128), jnp.float32),
            pltpu.VMEM((W // 256, 96, 32), jnp.float32),
            pltpu.VMEM((2, W // 256, 16, 32), jnp.float32),
            pltpu.SemaphoreType.DMA((4,)),
            pltpu.SemaphoreType.DMA((4,)),
            pltpu.SemaphoreType.DMA((2,)),
            pltpu.SemaphoreType.DMA((2,)),
            pltpu.SemaphoreType.DMA((3,)),
        ],
        compiler_params=pltpu.CompilerParams(collective_id=0, has_side_effects=True, vmem_limit_bytes=8 << 20),
        name="fit",
    )(points, source)


def render_kernel(first_ref, count_ref, fit_ref, num_ref, sp_s, low_s, far_s, ix_s, w0_s, w1_s, paged, wide_ref,
                  out_ref, aff_ref, halo, accum, num_m, sem):
    blocks = W // 128
    tile = lax.axis_index("ty")
    n = lax.axis_size("ty")
    f32 = jnp.float32
    bring = pltpu.make_async_copy(num_ref, num_m, sem)
    bring.start()
    for f in range(6):
        aff_ref[f] = fit_ref[8 * f + 1 : 8 * f + 5, :]

    page_rows(wide_ref.at[0], halo.at[0], tile > 0)
    page_rows(wide_ref.at[1], halo.at[1], tile < n - 1)
    slot = lax.broadcasted_iota(jnp.int32, (8, 3 * H), 1)
    first = jnp.broadcast_to(first_ref[...].reshape(1, 1), slot.shape) * BH - tile * H + H
    last = first + jnp.broadcast_to(count_ref[...].reshape(1, 1), slot.shape) * BH
    slot = jnp.where((slot >= first) & (slot < last), (slot - H).astype(f32), -1e6)

    def source_of(b):
        cols = pl.ds(pl.multiple_of(b * 128, 128), 256)
        window = [
            jnp.concatenate([halo[0, p, :, cols], paged[p, :, cols], halo[1, p, :, cols]], axis=0) for p in range(2)]
        lows = [low_s[b, 8 * g : 8 * g + 8, :][:, : 3 * H] for g in range(GROUPS)]
        return window, lows

    def pull(held, start, size):
        window, lows = held
        onehot = jnp.concatenate(
            [jnp.where(slot == lows[g] + (start + d), 1.0, 0.0) for g in range(GROUPS) for d in range(size)], axis=0)
        onehot = onehot.astype(jnp.bfloat16)
        return [jnp.dot(onehot, w, preferred_element_type=f32) for w in window]

    def blend(b, got, start, size, accs):
        out = []
        for g in range(GROUPS):
            r = slice(8 * g, 8 * g + 8)
            lanes_at = ix_s[b, 16 * g : 16 * g + 16, :]
            m = lanes_at & 127
            here = far_s[b, r, :] < 128.0
            rel = sp_s[b, r, :]
            totals = [None, None]
            for d in range(size):
                at = slice(8 * (g * size + d), 8 * (g * size + d) + 8)
                near, far = [
                    jnp.concatenate([tap[at, side] for tap in got], axis=0).astype(jnp.bfloat16)
                    for side in (slice(0, 128), slice(128, 256))
                ]
                near, far = pick(near, m).astype(f32), pick(far, m).astype(f32)
                ty = jnp.maximum(0.0, 1.0 - jnp.abs(rel - (start + d)))
                for p in range(2):
                    term = jnp.where(here, near[8 * p : 8 * p + 8], far[8 * p : 8 * p + 8]) * ty
                    totals[p] = term if d == 0 else totals[p] + term
            res = totals[0] * w0_s[b, r, :] + totals[1] * w1_s[b, r, :]
            out.append(res if accs[g] is None else accs[g] + res)
        return tuple(out)

    def paint(q, _):
        bs = [q * UB + j for j in range(UB)]
        gots = [pull(source_of(b), 0.0, FIRST) for b in bs]
        for b, got in zip(bs, gots):
            accum[b] = jnp.concatenate(blend(b, got, 0.0, FIRST, (None,) * GROUPS), axis=0)
        return 0

    lax.fori_loop(0, blocks // UB, paint, 0)
    bring.wait()

    @pl.when(num_m[0, blocks] > 0)
    def _():
        def again(b, _):
            def more(k, accs):
                start = (FIRST + MORE * k).astype(f32)
                return blend(b, pull(source_of(b), start, MORE), start, MORE, accs)

            @pl.when(num_m[0, b] > 0)
            def _():
                accs = tuple(accum[b, 8 * g : 8 * g + 8, :] for g in range(GROUPS))
                accum[b] = jnp.concatenate(lax.fori_loop(0, num_m[0, b], more, accs), axis=0)

            return 0

        lax.fori_loop(0, blocks, again, 0)

    def emit(b, _):
        out_ref[:, pl.ds(pl.multiple_of(b * 128, 128), 128)] = accum[b].astype(jnp.bfloat16)
        return 0
    lax.fori_loop(0, blocks, emit, 0, unroll=4)


def render(first, count, fitted):
    vm = pl.BlockSpec(memory_space=pltpu.VMEM)
    return pl.pallas_call(
        render_kernel,
        out_shape=(
            jax.ShapeDtypeStruct((H, W), jnp.bfloat16),
            jax.ShapeDtypeStruct((6, VR, VC), jnp.float32),
        ),
        in_specs=[vm] * (2 + len(fitted)),
        out_specs=(vm, vm),
        scratch_shapes=[
            pltpu.VMEM((2, 2, H, W + 128), jnp.bfloat16),
            pltpu.VMEM((W // 128, H, 128), jnp.float32),
            pltpu.SMEM((8, 128), jnp.int32),
            pltpu.SemaphoreType.DMA,
        ],
        compiler_params=pltpu.CompilerParams(vmem_limit_bytes=16 << 20),
        name="render",
    )(first, count, *fitted)


def per_device(points, source, slab_first, slab_count):
    points, source = [pltpu.with_memory_space_constraint(x, pltpu.HBM) for x in (points, source)]
    return render(slab_first, slab_count, fit(points, source))


def solution(mesh):
    return jax.shard_map(
        per_device,
        mesh=mesh,
        in_specs=(
            P(None, ("sec", "ty")),
            P(("sec", "ty"), None),
            P(("sec", "ty")),
            P(("sec", "ty")),
        ),
        out_specs=(P(("sec", "ty"), None), P(None, ("sec", "ty"), None)),
        check_vma=False,
    )
```

```python
import math

import jax
import jax.numpy as jnp
from jax import lax
from jax.experimental import pallas as pl
from jax.experimental.pallas import tpu as pltpu
from jax.sharding import PartitionSpec as P

W = 2048
BH = 16
SP = 8
H = 32
K = 6
VR = 4
VC = 256


MESH = pl.DeviceIdType.MESH
RIDGE_TERM = 0.01


def solve_affine(moments, vertex_x, vertex_y):
    scale = 1.0 / moments[0]
    mean_px, mean_py, mean_qx, mean_qy = [m * scale for m in moments[1:5]]
    cov_xx = moments[5] * scale - mean_px * mean_px + RIDGE_TERM
    cov_xy = moments[6] * scale - mean_px * mean_py
    cov_yy = moments[7] * scale - mean_py * mean_py + RIDGE_TERM
    cross_xx = moments[8] * scale - mean_qx * mean_px
    cross_xy = moments[9] * scale - mean_qx * mean_py
    cross_yx = moments[10] * scale - mean_qy * mean_px
    cross_yy = moments[11] * scale - mean_qy * mean_py
    inverse = 1.0 / (cov_xx * cov_yy - cov_xy * cov_xy)
    lin_xx = (cross_xx * cov_yy - cross_xy * cov_xy) * inverse
    lin_xy = (cross_xy * cov_xx - cross_xx * cov_xy) * inverse
    lin_yx = (cross_yx * cov_yy - cross_yy * cov_xy) * inverse
    lin_yy = (cross_yy * cov_xx - cross_yx * cov_xy) * inverse
    delta_x = vertex_x - mean_px
    delta_y = vertex_y - mean_py
    shift_x = mean_qx + lin_xx * delta_x + lin_xy * delta_y - vertex_x
    shift_y = mean_qy + lin_yx * delta_x + lin_yy * delta_y - vertex_y
    return [lin_xx, lin_xy, lin_yx, lin_yy, shift_x, shift_y]


GROUPS = H // SP
FIRST = 9
UB = 16
UP = 4
MORE = 2
PER = 7


def pick(x, lanes):
    dims = lax.GatherDimensionNumbers(
        offset_dims=(), collapsed_slice_dims=(1,), start_index_map=(1,),
        operand_batching_dims=(0,), start_indices_batching_dims=(0,))
    return lax.gather(x, lanes[..., None], dims, slice_sizes=(1, 1),
                      mode=lax.GatherScatterMode.PROMISE_IN_BOUNDS)


def page_rows(rows_ref, to, there):
    lanes = lax.broadcasted_iota(jnp.int32, (H, 128), 1)
    zero = jnp.zeros((H, 128), jnp.bfloat16)
    prev = [zero, zero]
    for k in range(W // 128 + 1):
        now = zero
        if k < W // 128:
            now = rows_ref[:, 128 * k : 128 * k + 128]
            if there is not None:
                now = jnp.where(there, now, zero)
        for p, turn in enumerate((64, 63)):
            turned = pltpu.roll(now, turn, 1) if k < W // 128 else zero
            to[p, :, 128 * k : 128 * k + 128] = jnp.where(lanes < turn, prev[p], turned)
            prev[p] = turned


def positions(shifts, ext, num_ref, sp_s, low_s, far_s, ix_s, w0_s, w1_s):
    blocks = W // 128
    f32 = jnp.float32
    left, right = shifts[:, 0:128], shifts[:, 128:256]
    lane16 = lax.broadcasted_iota(jnp.int32, (16, 128), 1)
    ext[0] = jnp.where(lane16 < 1, left[:, 0:1], pltpu.roll(left, 1, 1))
    ext[1] = jnp.where(lane16 < 17, pltpu.roll(left, 17, 1), pltpu.roll(right, 17, 1))
    ext[2] = jnp.where(lane16 < 33, pltpu.roll(right, 33, 1), right[:, 127:128])

    sub = lax.broadcasted_iota(jnp.int32, (8, 128), 0)
    subf = sub.astype(f32)
    lane = lax.broadcasted_iota(jnp.int32, (8, 128), 1)
    wa = jnp.maximum(0.0, 1.0 - (subf + 4.0) * (1.0 / SP))
    wb = jnp.maximum(0.0, 1.0 - jnp.abs(subf - 4.0) * (1.0 / SP))
    wc = jnp.maximum(0.0, 1.0 - (12.0 - subf) * (1.0 / SP))
    wa, wb, wc = H * wa, H * wb, H * wc
    column = lane.astype(f32) + 64.0
    step = (lane + SP // 2) // SP
    part = ((lane + SP // 2) % SP).astype(f32) * (1.0 / SP)

    def prepare(b, spans):
        page = b // PER
        at = step + (b - page * PER) * (128 // SP)
        fine = []
        for half in range(2):
            held = ext[page, 8 * half : 8 * half + 8, :]
            near = pick(held, at)
            fine.append(near + part * (pick(held, at + 1) - near))
        fx, fy = fine
        most = None
        for g in range(GROUPS):
            dx = wa * fx[g : g + 1] + wb * fx[g + 1 : g + 2] + wc * fx[g + 2 : g + 3]
            dy = wa * fy[g : g + 1] + wb * fy[g + 1 : g + 2] + wc * fy[g + 2 : g + 3]
            sy = jnp.clip((subf + 8.0 * g) + dy, -33.0, 64.0)
            lx = jnp.clip(column + dx, -1.0, 256.0)
            base = jnp.clip(jnp.floor(lx), 0.0, 255.0)
            past = lx - base
            taps = [1.0 - jnp.abs(past), jnp.maximum(jnp.minimum(past, 255.0 - base), 0.0)]
            low = jnp.floor(jnp.min(sy, axis=1, keepdims=True))
            rel = sy - low
            most = rel if most is None else jnp.maximum(most, rel)
            r, tall = slice(8 * g, 8 * g + 8), slice(16 * g, 16 * g + 16)
            sp_s[b, r, :] = rel
            low_s[b, r, :] = jnp.broadcast_to(low, (8, 128))
            far_s[b, r, :] = base
            at = base.astype(jnp.int32)
            ix_s[b, tall, :] = jnp.concatenate([at, at], axis=0).astype(jnp.int16)
            taps = jnp.concatenate(taps, axis=0).astype(jnp.bfloat16).astype(f32)
            w0_s[b, r, :] = taps[0:8]
            w1_s[b, r, :] = taps[8:16]
        return jnp.where(lane == b, jnp.max(most, axis=1, keepdims=True), spans)

    spans = jnp.zeros((8, 128), f32)
    for b in range(blocks):
        spans = prepare(b, spans)
    rows = jnp.floor(jnp.max(spans, axis=0, keepdims=True)).astype(jnp.int32) + 2
    extra = (jnp.maximum(rows - FIRST, 0) + (MORE - 1)) // MORE
    extra = jnp.where(lane[0:1] == blocks, jnp.max(extra, axis=1, keepdims=True), extra)
    num_ref[...] = jnp.broadcast_to(extra, (8, 128))


OFFSETS = (1, -1, 2, -2)
FAR = 1e5
RATE = -2.0 * math.log2(math.e)
SKIP = 1e3


def halves(x):
    high = x.astype(jnp.bfloat16)
    return high, (x - high.astype(jnp.float32)).astype(jnp.bfloat16)


def fit_kernel(pts_ref, src_ref, fit_ref, num_ref, sp_s, low_s, far_s, ix_s, w0_s, w1_s, paged, wide,
               rows_s, ext, held, staged, mom, side, send_p, recv_p, send_s, recv_s, load):
    f32 = jnp.float32
    me = lax.axis_index("ty")
    n = lax.axis_size("ty")
    half = pts_ref.shape[1] // 2
    pairs = W // 256

    def exists(d):
        return (me + d >= 0) & (me + d < n)

    own_points = [
        pltpu.make_async_copy(pts_ref.at[:, pl.ds(c * half, half)], held.at[2, pl.ds(4 * c, 4)], load.at[c])
        for c in range(2)
    ]
    for c in own_points:
        c.start()
    own_rows = pltpu.make_async_copy(src_ref, rows_s, load.at[2])
    own_rows.start()
    barrier = pltpu.get_barrier_semaphore()
    for d in OFFSETS:
        @pl.when(exists(d))
        def _(d=d):
            pl.semaphore_signal(barrier, inc=1, device_id={"ty": me + d}, device_id_type=MESH)
    peers = sum(exists(d).astype(jnp.int32) for d in OFFSETS)

    def points_to(i, d):
        return pltpu.make_async_remote_copy(
            src_ref=held.at[2], dst_ref=held.at[2 - d], send_sem=send_p.at[i], recv_sem=recv_p.at[i],
            device_id={"ty": me + d}, device_id_type=MESH)

    def source_to(i, d):
        return pltpu.make_async_remote_copy(
            src_ref=src_ref, dst_ref=wide.at[i], send_sem=send_s.at[i], recv_sem=recv_s.at[i],
            device_id={"ty": me + d}, device_id_type=MESH)

    for c in own_points:
        c.wait()
    pl.semaphore_wait(barrier, peers)
    for i, d in enumerate(OFFSETS):
        @pl.when(exists(d))
        def _(i=i, d=d):
            points_to(i, d).start()
    for i, d in enumerate(OFFSETS[:2]):
        @pl.when(exists(d))
        def _(i=i, d=d):
            source_to(i, d).start()

    wide_lane = lax.broadcasted_iota(jnp.int32, (8, half + 128), 1) // 128
    wide_row = lax.broadcasted_iota(jnp.int32, (8, half + 128), 0) % 2
    centre = (me * H).astype(f32) + H / 2.0
    anchors = [
        jnp.where(wide_row == 0, ((2 * wide_lane + odd) * 256 + 128).astype(f32), centre) * (1.0 / H)
        for odd in range(2)
    ]
    spare = jnp.full((8, 128), FAR, f32)

    def stage(tile):
        data = held[2] if tile == 2 else jnp.where(exists(tile - 2), held[tile], FAR)
        row = jnp.concatenate([data, spare], axis=1) * (1.0 / H)
        staged[0, tile] = pltpu.roll(row, 32, 1) - anchors[0]
        staged[1, tile] = pltpu.roll(row, half + 96, 1) - anchors[1]

    e = lax.broadcasted_iota(jnp.int32, (8, 128), 0)
    vy = (((e - 1) * SP + SP // 2) - H // 2).astype(f32) * (1.0 / H)
    vy_of = {1: jnp.where(e == 5, SKIP, vy), 2: vy, 3: jnp.where(e == 0, SKIP, vy)}
    lone = {0: (-SP // 2 - H // 2) / H, 4: (4 * SP + SP // 2 - H // 2) / H}
    lane32 = lax.broadcasted_iota(jnp.int32, (32, 128), 1)
    vert32 = lax.broadcasted_iota(jnp.int32, (32, 128), 0)
    near = jnp.abs(lane32 // 32 - 1 - vert32 // 16) <= 1
    vx = jnp.where(near, (vert32 * SP + SP // 2 - 128).astype(f32) * (1.0 / H), SKIP)

    def bell(gap):
        return jnp.exp2((gap * gap) * RATE)

    def rows_of(k, odd, tile, c):
        at = pl.ds(pl.multiple_of(k * 128, 128), 128)
        return [jnp.broadcast_to(staged[odd, tile, 4 * c + i : 4 * c + i + 1, at], (8, 128)) for i in range(4)]

    def across(px):
        gap = jnp.concatenate([px - vx[8 * g : 8 * g + 8] for g in range(4)], axis=0)
        return jnp.concatenate(halves(bell(gap)), axis=0)

    def contract(parts, weights):
        return lax.dot_general(
            jnp.concatenate(parts, axis=1), jnp.concatenate(weights, axis=1),
            (((1,), (1,)), ((), ())), preferred_element_type=f32)

    def dense(k, odd, tiles):
        parts, weights = [], []
        for tile in tiles:
            for c in range(2):
                px, py, qx, qy = rows_of(k, odd, tile, c)
                weights.append(across(px))
                w = bell(py - vy_of[tile])
                wpx = w * px
                wpy = w * py
                feats = jnp.concatenate(
                    [w, wpx, wpy, w * qx, w * qy, wpx * px, wpx * py, wpy * py,
                     wpx * qx, wpy * qx, wpx * qy, wpy * qy], axis=0)
                parts.append(jnp.concatenate(halves(feats), axis=0))
        got = contract(parts, weights)
        got = got[0:96] + got[96:192]
        return got[:, 0:32] + got[:, 32:64]

    def single(k, odd, tile):
        parts, weights = [], []
        for c in range(2):
            px, py, qx, qy = rows_of(k, odd, tile, c)
            weights.append(across(px))
            w = bell(py - lone[tile])
            a1 = jnp.where(e == 0, 1.0, jnp.where((e == 2) | (e == 7), py, jnp.where(e == 3, qx, jnp.where(e == 4, qy, px))))
            b1 = jnp.where(e < 5, 1.0, jnp.where(e == 5, px, py))
            a2 = jnp.where(e % 2 == 0, px, py)
            b2 = jnp.where(e < 2, qx, qy)
            feats = jnp.concatenate([w * a1 * b1, w * a2 * b2], axis=0)
            parts.append(jnp.concatenate(halves(feats), axis=0))
        got = contract(parts, weights)
        got = got[0:16] + got[16:32]
        return got[:, 0:32] + got[:, 32:64]

    def own_group(k, _):
        for odd in range(2):
            mom[2 * k + odd] = dense(k, odd, (2,))
        return 0

    def next_group(k, _):
        for odd in range(2):
            mom[2 * k + odd] += dense(k, odd, (1, 3))
        return 0

    def last_group(k, _):
        for odd in range(2):
            for s, tile in enumerate((0, 4)):
                side[s, 2 * k + odd] = single(k, odd, tile)
        return 0

    def arrive(which):
        for i in which:
            @pl.when(exists(-OFFSETS[i]))
            def _(i=i):
                points_to(i, OFFSETS[i]).wait_recv()
        for i in which:
            stage(2 - OFFSETS[i])

    stage(2)
    lax.fori_loop(0, pairs // 2, own_group, 0, unroll=4)
    own_rows.wait()
    page_rows(rows_s, paged, None)
    arrive((0, 1))
    lax.fori_loop(0, pairs // 2, next_group, 0, unroll=4)
    arrive((2, 3))
    lax.fori_loop(0, pairs // 2, last_group, 0, unroll=4)

    ew = lax.broadcasted_iota(jnp.int32, (8, VC), 0)
    jw = lax.broadcasted_iota(jnp.int32, (8, VC), 1)
    vertex_y = (((ew - 1) * SP + SP // 2) - H // 2).astype(f32) * (1.0 / H)
    vertex_x = ((jw % 32) * SP + SP // 2 - 128).astype(f32) * (1.0 / H)
    safe = ew < 6
    sides = [jnp.concatenate([side[s, g] for g in range(pairs)], axis=1) for s in range(2)]
    moments = []
    for f in range(12):
        m = jnp.concatenate([mom[g, 8 * f : 8 * f + 8, :] for g in range(pairs)], axis=1)
        m = m + jnp.where(ew == 0, sides[0][f : f + 1], jnp.where(ew == 5, sides[1][f : f + 1], 0.0))
        moments.append(m)
    moments[0] = jnp.where(safe, moments[0], 1.0)
    solved = solve_affine(moments, vertex_x, vertex_y)
    for f in range(6):
        x = solved[f]
        if f >= 4:
            x = jnp.where((ew == 0) & (me == 0), x[1:2], x)
            x = jnp.where((ew == 5) & (me == n - 1), x[4:5], x)
            x = jnp.where(safe, x, 0.0)
        fit_ref[8 * f : 8 * f + 8, :] = x
        solved[f] = x
    positions(jnp.concatenate(solved[4:6], axis=0), ext, num_ref, sp_s, low_s, far_s, ix_s, w0_s, w1_s)

    for i, d in enumerate(OFFSETS[:2]):
        @pl.when(exists(-d))
        def _(i=i, d=d):
            source_to(i, d).wait_recv()
    for i, d in enumerate(OFFSETS):
        @pl.when(exists(d))
        def _(i=i, d=d):
            points_to(i, d).wait_send()
    for i, d in enumerate(OFFSETS[:2]):
        @pl.when(exists(d))
        def _(i=i, d=d):
            source_to(i, d).wait_send()


def fit(points, source):
    size = points.shape[1]
    blocks = W // 128
    per = lambda d: pltpu.VMEM((blocks, H, 128), d)
    vm = pl.BlockSpec(memory_space=pltpu.VMEM)
    return pl.pallas_call(
        fit_kernel,
        out_shape=(
            pltpu.VMEM((48, VC), jnp.float32),
            pltpu.VMEM((8, 128), jnp.int32),
            per(jnp.float32), per(jnp.float32), per(jnp.float32),
            pltpu.VMEM((blocks, 2 * H, 128), jnp.int16),
            per(jnp.float32), per(jnp.float32),
            pltpu.VMEM((2, H, W + 128), jnp.bfloat16),
            pltpu.VMEM((2, H, W), jnp.bfloat16),
        ),
        in_specs=[pl.BlockSpec(memory_space=pltpu.HBM)] * 2,
        out_specs=(vm,) * 10,
        scratch_shapes=[
            pltpu.VMEM((H, W), jnp.bfloat16),
            pltpu.VMEM((-(-blocks // PER), 16, 128), jnp.float32),
            pltpu.VMEM((5, 8, size // 2), jnp.float32),
            pltpu.VMEM((2, 5, 8, size // 2 + 128), jnp.float32),
            pltpu.VMEM((W // 256, 96, 32), jnp.float32),
            pltpu.VMEM((2, W // 256, 16, 32), jnp.float32),
            pltpu.SemaphoreType.DMA((4,)),
            pltpu.SemaphoreType.DMA((4,)),
            pltpu.SemaphoreType.DMA((2,)),
            pltpu.SemaphoreType.DMA((2,)),
            pltpu.SemaphoreType.DMA((3,)),
        ],
        compiler_params=pltpu.CompilerParams(collective_id=0, has_side_effects=True, vmem_limit_bytes=8 << 20),
        name="fit",
    )(points, source)


def render_kernel(first_ref, count_ref, fit_ref, num_ref, sp_s, low_s, far_s, ix_s, w0_s, w1_s, paged, wide_ref,
                  out_ref, aff_ref, halo, accum, num_m, sem):
    blocks = W // 128
    tile = lax.axis_index("ty")
    n = lax.axis_size("ty")
    f32 = jnp.float32
    bring = pltpu.make_async_copy(num_ref, num_m, sem)
    bring.start()
    for f in range(6):
        aff_ref[f] = fit_ref[8 * f + 1 : 8 * f + 5, :]

    page_rows(wide_ref.at[0], halo.at[0], tile > 0)
    page_rows(wide_ref.at[1], halo.at[1], tile < n - 1)
    slot = lax.broadcasted_iota(jnp.int32, (8, 3 * H), 1)
    first = jnp.broadcast_to(first_ref[...].reshape(1, 1), slot.shape) * BH - tile * H + H
    last = first + jnp.broadcast_to(count_ref[...].reshape(1, 1), slot.shape) * BH
    slot = jnp.where((slot >= first) & (slot < last), (slot - H).astype(f32), -1e6)

    def source_of(b):
        cols = pl.ds(pl.multiple_of(b * 128, 128), 256)
        window = [
            jnp.concatenate([halo[0, p, :, cols], paged[p, :, cols], halo[1, p, :, cols]], axis=0) for p in range(2)]
        lows = [slot - low_s[b, 8 * g : 8 * g + 8, :][:, : 3 * H] for g in range(GROUPS)]
        return window, lows

    def pull(held, start, size):
        window, lows = held
        onehot = jnp.concatenate(
            [jnp.where(lows[g] == start + d, 1.0, 0.0) for g in range(GROUPS) for d in range(size)], axis=0)
        onehot = onehot.astype(jnp.bfloat16)
        return [jnp.dot(onehot, w, preferred_element_type=f32) for w in window]

    def blend(b, got, start, size, accs):
        out = []
        for g in range(GROUPS):
            r = slice(8 * g, 8 * g + 8)
            lanes_at = ix_s[b, 16 * g : 16 * g + 16, :]
            m = lanes_at & 127
            here = far_s[b, r, :] < 128.0
            rel = sp_s[b, r, :]
            totals = [None, None]
            last = jnp.clip(rel - (start - 1.0), 0.0, 1.0)
            for d in range(size):
                at = slice(8 * (g * size + d), 8 * (g * size + d) + 8)
                near, far = [
                    jnp.concatenate([tap[at, side] for tap in got], axis=0).astype(jnp.bfloat16)
                    for side in (slice(0, 128), slice(128, 256))
                ]
                near, far = pick(near, m).astype(f32), pick(far, m).astype(f32)
                ramp = jnp.clip(rel - (start + d), 0.0, 1.0)
                ty = last - ramp
                last = ramp
                for p in range(2):
                    term = jnp.where(here, near[8 * p : 8 * p + 8], far[8 * p : 8 * p + 8]) * ty
                    totals[p] = term if d == 0 else totals[p] + term
            res = totals[0] * w0_s[b, r, :] + totals[1] * w1_s[b, r, :]
            out.append(res if accs[g] is None else accs[g] + res)
        return tuple(out)

    def put(b, rows):
        rows = jnp.concatenate(rows, axis=0)
        accum[b] = rows
        out_ref[:, pl.ds(b * 128 if isinstance(b, int) else pl.multiple_of(b * 128, 128), 128)] = rows.astype(jnp.bfloat16)

    def paint(q, _):
        bs = [q * UB + j for j in range(UB)]
        gots = [pull(source_of(b), 0.0, FIRST) for b in bs]
        for b, got in zip(bs, gots):
            put(b, blend(b, got, 0.0, FIRST, (None,) * GROUPS))
        return 0

    lax.fori_loop(0, blocks // UB, paint, 0)
    bring.wait()

    @pl.when(num_m[0, blocks] > 0)
    def _():
        def again(b, _):
            def more(k, accs):
                start = (FIRST + MORE * k).astype(f32)
                return blend(b, pull(source_of(b), start, MORE), start, MORE, accs)

            @pl.when(num_m[0, b] > 0)
            def _():
                accs = tuple(accum[b, 8 * g : 8 * g + 8, :] for g in range(GROUPS))
                put(b, lax.fori_loop(0, num_m[0, b], more, accs))

            return 0

        lax.fori_loop(0, blocks, again, 0)


def render(first, count, fitted):
    vm = pl.BlockSpec(memory_space=pltpu.VMEM)
    return pl.pallas_call(
        render_kernel,
        out_shape=(
            jax.ShapeDtypeStruct((H, W), jnp.bfloat16),
            jax.ShapeDtypeStruct((6, VR, VC), jnp.float32),
        ),
        in_specs=[vm] * (2 + len(fitted)),
        out_specs=(vm, vm),
        scratch_shapes=[
            pltpu.VMEM((2, 2, H, W + 128), jnp.bfloat16),
            pltpu.VMEM((W // 128, H, 128), jnp.float32),
            pltpu.SMEM((8, 128), jnp.int32),
            pltpu.SemaphoreType.DMA,
        ],
        compiler_params=pltpu.CompilerParams(vmem_limit_bytes=16 << 20),
        name="render",
    )(first, count, *fitted)


def per_device(points, source, slab_first, slab_count):
    points, source = [pltpu.with_memory_space_constraint(x, pltpu.HBM) for x in (points, source)]
    return render(slab_first, slab_count, fit(points, source))


def solution(mesh):
    return jax.shard_map(
        per_device,
        mesh=mesh,
        in_specs=(
            P(None, ("sec", "ty")),
            P(("sec", "ty"), None),
            P(("sec", "ty")),
            P(("sec", "ty")),
        ),
        out_specs=(P(("sec", "ty"), None), P(None, ("sec", "ty"), None)),
        check_vma=False,
    )
```

```python
import math

import jax
import jax.numpy as jnp
from jax import lax
from jax.experimental import pallas as pl
from jax.experimental.pallas import tpu as pltpu
from jax.sharding import PartitionSpec as P

W = 2048
BH = 16
SP = 8
H = 32
K = 6
VR = 4
VC = 256


MESH = pl.DeviceIdType.MESH
RIDGE_TERM = 0.01


def solve_affine(moments, vertex_x, vertex_y):
    scale = 1.0 / moments[0]
    mean_px, mean_py, mean_qx, mean_qy = [m * scale for m in moments[1:5]]
    cov_xx = moments[5] * scale - mean_px * mean_px + RIDGE_TERM
    cov_xy = moments[6] * scale - mean_px * mean_py
    cov_yy = moments[7] * scale - mean_py * mean_py + RIDGE_TERM
    cross_xx = moments[8] * scale - mean_qx * mean_px
    cross_xy = moments[9] * scale - mean_qx * mean_py
    cross_yx = moments[10] * scale - mean_qy * mean_px
    cross_yy = moments[11] * scale - mean_qy * mean_py
    inverse = 1.0 / (cov_xx * cov_yy - cov_xy * cov_xy)
    lin_xx = (cross_xx * cov_yy - cross_xy * cov_xy) * inverse
    lin_xy = (cross_xy * cov_xx - cross_xx * cov_xy) * inverse
    lin_yx = (cross_yx * cov_yy - cross_yy * cov_xy) * inverse
    lin_yy = (cross_yy * cov_xx - cross_yx * cov_xy) * inverse
    delta_x = vertex_x - mean_px
    delta_y = vertex_y - mean_py
    shift_x = mean_qx + lin_xx * delta_x + lin_xy * delta_y - vertex_x
    shift_y = mean_qy + lin_yx * delta_x + lin_yy * delta_y - vertex_y
    return [lin_xx, lin_xy, lin_yx, lin_yy, shift_x, shift_y]


GROUPS = H // SP
FIRST = 9
UB = 16
UP = 4
MORE = 2
PER = 7


def pick(x, lanes):
    dims = lax.GatherDimensionNumbers(
        offset_dims=(), collapsed_slice_dims=(1,), start_index_map=(1,),
        operand_batching_dims=(0,), start_indices_batching_dims=(0,))
    return lax.gather(x, lanes[..., None], dims, slice_sizes=(1, 1),
                      mode=lax.GatherScatterMode.PROMISE_IN_BOUNDS)


def page_rows(rows_ref, to, there):
    lanes = lax.broadcasted_iota(jnp.int32, (H, 128), 1)
    zero = jnp.zeros((H, 128), jnp.bfloat16)
    prev = [zero, zero]
    for k in range(W // 128 + 1):
        now = zero
        if k < W // 128:
            now = rows_ref[:, 128 * k : 128 * k + 128]
            if there is not None:
                now = jnp.where(there, now, zero)
        for p, turn in enumerate((64, 63)):
            turned = pltpu.roll(now, turn, 1) if k < W // 128 else zero
            to[p, :, 128 * k : 128 * k + 128] = jnp.where(lanes < turn, prev[p], turned)
            prev[p] = turned


def positions(shifts, ext, num_ref, sp_s, low_s, far_s, ix_s, w0_s, w1_s):
    blocks = W // 128
    f32 = jnp.float32
    left, right = shifts[:, 0:128], shifts[:, 128:256]
    lane16 = lax.broadcasted_iota(jnp.int32, (16, 128), 1)
    ext[0] = jnp.where(lane16 < 1, left[:, 0:1], pltpu.roll(left, 1, 1))
    ext[1] = jnp.where(lane16 < 17, pltpu.roll(left, 17, 1), pltpu.roll(right, 17, 1))
    ext[2] = jnp.where(lane16 < 33, pltpu.roll(right, 33, 1), right[:, 127:128])

    sub = lax.broadcasted_iota(jnp.int32, (8, 128), 0)
    subf = sub.astype(f32)
    lane = lax.broadcasted_iota(jnp.int32, (8, 128), 1)
    wa = jnp.maximum(0.0, 1.0 - (subf + 4.0) * (1.0 / SP))
    wb = jnp.maximum(0.0, 1.0 - jnp.abs(subf - 4.0) * (1.0 / SP))
    wc = jnp.maximum(0.0, 1.0 - (12.0 - subf) * (1.0 / SP))
    wa, wb, wc = H * wa, H * wb, H * wc
    column = lane.astype(f32) + 64.0
    step = (lane + SP // 2) // SP
    part = ((lane + SP // 2) % SP).astype(f32) * (1.0 / SP)

    def prepare(b, spans):
        page = b // PER
        at = step + (b - page * PER) * (128 // SP)
        fine = []
        for half in range(2):
            held = ext[page, 8 * half : 8 * half + 8, :]
            near = pick(held, at)
            fine.append(near + part * (pick(held, at + 1) - near))
        fx, fy = fine
        most = None
        for g in range(GROUPS):
            dx = wa * fx[g : g + 1] + wb * fx[g + 1 : g + 2] + wc * fx[g + 2 : g + 3]
            dy = wa * fy[g : g + 1] + wb * fy[g + 1 : g + 2] + wc * fy[g + 2 : g + 3]
            sy = jnp.clip((subf + 8.0 * g) + dy, -33.0, 64.0)
            lx = jnp.clip(column + dx, -1.0, 256.0)
            base = jnp.clip(jnp.floor(lx), 0.0, 255.0)
            past = lx - base
            taps = [1.0 - jnp.abs(past), jnp.maximum(jnp.minimum(past, 255.0 - base), 0.0)]
            low = jnp.floor(jnp.min(sy, axis=1, keepdims=True))
            rel = sy - low
            most = rel if most is None else jnp.maximum(most, rel)
            r, tall = slice(8 * g, 8 * g + 8), slice(16 * g, 16 * g + 16)
            sp_s[b, r, :] = rel
            low_s[b, r, :] = jnp.broadcast_to(low, (8, 128))
            far_s[b, r, :] = base
            at = base.astype(jnp.int32)
            ix_s[b, tall, :] = jnp.concatenate([at, at], axis=0).astype(jnp.int16)
            taps = jnp.concatenate(taps, axis=0).astype(jnp.bfloat16).astype(f32)
            w0_s[b, r, :] = taps[0:8]
            w1_s[b, r, :] = taps[8:16]
        return jnp.where(lane == b, jnp.max(most, axis=1, keepdims=True), spans)

    spans = jnp.zeros((8, 128), f32)
    for b in range(blocks):
        spans = prepare(b, spans)
    rows = jnp.floor(jnp.max(spans, axis=0, keepdims=True)).astype(jnp.int32) + 2
    extra = (jnp.maximum(rows - FIRST, 0) + (MORE - 1)) // MORE
    extra = jnp.where(lane[0:1] == blocks, jnp.max(extra, axis=1, keepdims=True), extra)
    num_ref[...] = jnp.broadcast_to(extra, (8, 128))


OFFSETS = (1, -1, 2, -2)
FAR = 1e5
RATE = -2.0 * math.log2(math.e)
SKIP = 1e3


def halves(x):
    high = x.astype(jnp.bfloat16)
    return high, (x - high.astype(jnp.float32)).astype(jnp.bfloat16)


def fit_kernel(pts_ref, src_ref, fit_ref, num_ref, sp_s, low_s, far_s, ix_s, w0_s, w1_s, paged, wide,
               rows_s, ext, held, staged, mom, side, send_p, recv_p, send_s, recv_s, load):
    f32 = jnp.float32
    me = lax.axis_index("ty")
    n = lax.axis_size("ty")
    half = pts_ref.shape[1] // 2
    pairs = W // 256

    def exists(d):
        return (me + d >= 0) & (me + d < n)

    own_points = [
        pltpu.make_async_copy(pts_ref.at[:, pl.ds(c * half, half)], held.at[2, pl.ds(4 * c, 4)], load.at[c])
        for c in range(2)
    ]
    for c in own_points:
        c.start()
    own_rows = pltpu.make_async_copy(src_ref, rows_s, load.at[2])
    own_rows.start()
    barrier = pltpu.get_barrier_semaphore()
    for d in OFFSETS:
        @pl.when(exists(d))
        def _(d=d):
            pl.semaphore_signal(barrier, inc=1, device_id={"ty": me + d}, device_id_type=MESH)
    peers = sum(exists(d).astype(jnp.int32) for d in OFFSETS)

    def points_to(i, d):
        return pltpu.make_async_remote_copy(
            src_ref=held.at[2], dst_ref=held.at[2 - d], send_sem=send_p.at[i], recv_sem=recv_p.at[i],
            device_id={"ty": me + d}, device_id_type=MESH)

    def source_to(i, d):
        return pltpu.make_async_remote_copy(
            src_ref=src_ref, dst_ref=wide.at[i], send_sem=send_s.at[i], recv_sem=recv_s.at[i],
            device_id={"ty": me + d}, device_id_type=MESH)

    for c in own_points:
        c.wait()
    pl.semaphore_wait(barrier, peers)
    for i, d in enumerate(OFFSETS):
        @pl.when(exists(d))
        def _(i=i, d=d):
            points_to(i, d).start()
    for i, d in enumerate(OFFSETS[:2]):
        @pl.when(exists(d))
        def _(i=i, d=d):
            source_to(i, d).start()

    wide_lane = lax.broadcasted_iota(jnp.int32, (8, half + 128), 1) // 128
    wide_row = lax.broadcasted_iota(jnp.int32, (8, half + 128), 0) % 2
    centre = (me * H).astype(f32) + H / 2.0
    anchors = [
        jnp.where(wide_row == 0, ((2 * wide_lane + odd) * 256 + 128).astype(f32), centre) * (1.0 / H)
        for odd in range(2)
    ]
    spare = jnp.full((8, 128), FAR, f32)

    def stage(tile):
        data = held[2] if tile == 2 else jnp.where(exists(tile - 2), held[tile], FAR)
        row = jnp.concatenate([data, spare], axis=1) * (1.0 / H)
        staged[0, tile] = pltpu.roll(row, 32, 1) - anchors[0]
        staged[1, tile] = pltpu.roll(row, half + 96, 1) - anchors[1]

    e = lax.broadcasted_iota(jnp.int32, (8, 128), 0)
    vy = (((e - 1) * SP + SP // 2) - H // 2).astype(f32) * (1.0 / H)
    vy_of = {1: jnp.where(e == 5, SKIP, vy), 2: vy, 3: jnp.where(e == 0, SKIP, vy)}
    lone = {0: (-SP // 2 - H // 2) / H, 4: (4 * SP + SP // 2 - H // 2) / H}
    lane32 = lax.broadcasted_iota(jnp.int32, (32, 128), 1)
    vert32 = lax.broadcasted_iota(jnp.int32, (32, 128), 0)
    near = jnp.abs(lane32 // 32 - 1 - vert32 // 16) <= 1
    vx = jnp.where(near, (vert32 * SP + SP // 2 - 128).astype(f32) * (1.0 / H), SKIP)

    def bell(gap):
        return jnp.exp2((gap * gap) * RATE)

    def rows_of(k, odd, tile, c):
        at = pl.ds(pl.multiple_of(k * 128, 128), 128)
        return [jnp.broadcast_to(staged[odd, tile, 4 * c + i : 4 * c + i + 1, at], (8, 128)) for i in range(4)]

    def across(px):
        gap = jnp.concatenate([px - vx[8 * g : 8 * g + 8] for g in range(4)], axis=0)
        return jnp.concatenate(halves(bell(gap)), axis=0)

    def contract(parts, weights):
        return lax.dot_general(
            jnp.concatenate(parts, axis=1), jnp.concatenate(weights, axis=1),
            (((1,), (1,)), ((), ())), preferred_element_type=f32)

    def dense(k, odd, tiles):
        parts, weights = [], []
        for tile in tiles:
            for c in range(2):
                px, py, qx, qy = rows_of(k, odd, tile, c)
                weights.append(across(px))
                w = bell(py - vy_of[tile])
                wpx = w * px
                wpy = w * py
                feats = jnp.concatenate(
                    [w, wpx, wpy, w * qx, w * qy, wpx * px, wpx * py, wpy * py,
                     wpx * qx, wpy * qx, wpx * qy, wpy * qy], axis=0)
                parts.append(jnp.concatenate(halves(feats), axis=0))
        got = contract(parts, weights)
        got = got[0:96] + got[96:192]
        return got[:, 0:32] + got[:, 32:64]

    def single(k, odd, tile):
        parts, weights = [], []
        for c in range(2):
            px, py, qx, qy = rows_of(k, odd, tile, c)
            weights.append(across(px))
            w = bell(py - lone[tile])
            a1 = jnp.where(e == 0, 1.0, jnp.where((e == 2) | (e == 7), py, jnp.where(e == 3, qx, jnp.where(e == 4, qy, px))))
            b1 = jnp.where(e < 5, 1.0, jnp.where(e == 5, px, py))
            a2 = jnp.where(e % 2 == 0, px, py)
            b2 = jnp.where(e < 2, qx, qy)
            feats = jnp.concatenate([w * a1 * b1, w * a2 * b2], axis=0)
            parts.append(jnp.concatenate(halves(feats), axis=0))
        got = contract(parts, weights)
        got = got[0:16] + got[16:32]
        return got[:, 0:32] + got[:, 32:64]

    def own_group(k, _):
        for odd in range(2):
            mom[2 * k + odd] = dense(k, odd, (2,))
        return 0

    def next_group(k, _):
        for odd in range(2):
            mom[2 * k + odd] += dense(k, odd, (1, 3))
        return 0

    def last_group(k, _):
        for odd in range(2):
            for s, tile in enumerate((0, 4)):
                side[s, 2 * k + odd] = single(k, odd, tile)
        return 0

    def arrive(which):
        for i in which:
            @pl.when(exists(-OFFSETS[i]))
            def _(i=i):
                points_to(i, OFFSETS[i]).wait_recv()
        for i in which:
            stage(2 - OFFSETS[i])

    stage(2)
    lax.fori_loop(0, pairs // 2, own_group, 0, unroll=4)
    own_rows.wait()
    page_rows(rows_s, paged, None)
    arrive((0, 1))
    lax.fori_loop(0, pairs // 2, next_group, 0, unroll=4)
    arrive((2, 3))
    lax.fori_loop(0, pairs // 2, last_group, 0, unroll=4)

    ew = lax.broadcasted_iota(jnp.int32, (8, VC), 0)
    jw = lax.broadcasted_iota(jnp.int32, (8, VC), 1)
    vertex_y = (((ew - 1) * SP + SP // 2) - H // 2).astype(f32) * (1.0 / H)
    vertex_x = ((jw % 32) * SP + SP // 2 - 128).astype(f32) * (1.0 / H)
    safe = ew < 6
    sides = [jnp.concatenate([side[s, g] for g in range(pairs)], axis=1) for s in range(2)]
    moments = []
    for f in range(12):
        m = jnp.concatenate([mom[g, 8 * f : 8 * f + 8, :] for g in range(pairs)], axis=1)
        m = m + jnp.where(ew == 0, sides[0][f : f + 1], jnp.where(ew == 5, sides[1][f : f + 1], 0.0))
        moments.append(m)
    moments[0] = jnp.where(safe, moments[0], 1.0)
    solved = solve_affine(moments, vertex_x, vertex_y)
    for f in range(6):
        x = solved[f]
        if f >= 4:
            x = jnp.where((ew == 0) & (me == 0), x[1:2], x)
            x = jnp.where((ew == 5) & (me == n - 1), x[4:5], x)
            x = jnp.where(safe, x, 0.0)
        fit_ref[8 * f : 8 * f + 8, :] = x
        solved[f] = x
    positions(jnp.concatenate(solved[4:6], axis=0), ext, num_ref, sp_s, low_s, far_s, ix_s, w0_s, w1_s)

    for i, d in enumerate(OFFSETS[:2]):
        @pl.when(exists(-d))
        def _(i=i, d=d):
            source_to(i, d).wait_recv()
    for i, d in enumerate(OFFSETS):
        @pl.when(exists(d))
        def _(i=i, d=d):
            points_to(i, d).wait_send()
    for i, d in enumerate(OFFSETS[:2]):
        @pl.when(exists(d))
        def _(i=i, d=d):
            source_to(i, d).wait_send()


def fit(points, source):
    size = points.shape[1]
    blocks = W // 128
    per = lambda d: pltpu.VMEM((blocks, H, 128), d)
    vm = pl.BlockSpec(memory_space=pltpu.VMEM)
    return pl.pallas_call(
        fit_kernel,
        out_shape=(
            pltpu.VMEM((48, VC), jnp.float32),
            pltpu.VMEM((8, 128), jnp.int32),
            per(jnp.float32), per(jnp.float32), per(jnp.float32),
            pltpu.VMEM((blocks, 2 * H, 128), jnp.int16),
            per(jnp.float32), per(jnp.float32),
            pltpu.VMEM((2, H, W + 128), jnp.bfloat16),
            pltpu.VMEM((2, H, W), jnp.bfloat16),
        ),
        in_specs=[pl.BlockSpec(memory_space=pltpu.HBM)] * 2,
        out_specs=(vm,) * 10,
        scratch_shapes=[
            pltpu.VMEM((H, W), jnp.bfloat16),
            pltpu.VMEM((-(-blocks // PER), 16, 128), jnp.float32),
            pltpu.VMEM((5, 8, size // 2), jnp.float32),
            pltpu.VMEM((2, 5, 8, size // 2 + 128), jnp.float32),
            pltpu.VMEM((W // 256, 96, 32), jnp.float32),
            pltpu.VMEM((2, W // 256, 16, 32), jnp.float32),
            pltpu.SemaphoreType.DMA((4,)),
            pltpu.SemaphoreType.DMA((4,)),
            pltpu.SemaphoreType.DMA((2,)),
            pltpu.SemaphoreType.DMA((2,)),
            pltpu.SemaphoreType.DMA((3,)),
        ],
        compiler_params=pltpu.CompilerParams(collective_id=0, has_side_effects=True, vmem_limit_bytes=8 << 20),
        name="fit",
    )(points, source)


def render_kernel(first_ref, count_ref, fit_ref, num_ref, sp_s, low_s, far_s, ix_s, w0_s, w1_s, paged, wide_ref,
                  out_ref, aff_ref, halo, accum, num_m, sem):
    blocks = W // 128
    tile = lax.axis_index("ty")
    n = lax.axis_size("ty")
    f32 = jnp.float32
    bring = pltpu.make_async_copy(num_ref, num_m, sem)
    bring.start()
    for f in range(6):
        aff_ref[f] = fit_ref[8 * f + 1 : 8 * f + 5, :]

    page_rows(wide_ref.at[0], halo.at[0], tile > 0)
    page_rows(wide_ref.at[1], halo.at[1], tile < n - 1)
    slot = lax.broadcasted_iota(jnp.int32, (8, 3 * H), 1)
    first = jnp.broadcast_to(first_ref[...].reshape(1, 1), slot.shape) * BH - tile * H + H
    last = first + jnp.broadcast_to(count_ref[...].reshape(1, 1), slot.shape) * BH
    slot = jnp.where((slot >= first) & (slot < last), (slot - H).astype(f32), -1e6)

    def source_of(b):
        cols = pl.ds(b * 128 if isinstance(b, int) else pl.multiple_of(b * 128, 128), 256)
        window = [
            jnp.concatenate([halo[0, p, :, cols], paged[p, :, cols], halo[1, p, :, cols]], axis=0) for p in range(2)]
        lows = [slot - low_s[b, 8 * g : 8 * g + 8, :][:, : 3 * H] for g in range(GROUPS)]
        return window, lows

    def pull(held, start, size):
        window, lows = held
        onehot = jnp.concatenate(
            [jnp.where(lows[g] == start + d, 1.0, 0.0) for g in range(GROUPS) for d in range(size)], axis=0)
        onehot = onehot.astype(jnp.bfloat16)
        return [jnp.dot(onehot, w, preferred_element_type=f32) for w in window]

    def blend(b, got, start, size, accs):
        out = []
        for g in range(GROUPS):
            r = slice(8 * g, 8 * g + 8)
            lanes_at = ix_s[b, 16 * g : 16 * g + 16, :]
            m = lanes_at & 127
            here = far_s[b, r, :] < 128.0
            rel = sp_s[b, r, :]
            totals = [None, None]
            last = jnp.clip(rel - (start - 1.0), 0.0, 1.0)
            for d in range(size):
                at = slice(8 * (g * size + d), 8 * (g * size + d) + 8)
                near, far = [
                    jnp.concatenate([tap[at, side] for tap in got], axis=0).astype(jnp.bfloat16)
                    for side in (slice(0, 128), slice(128, 256))
                ]
                near, far = pick(near, m).astype(f32), pick(far, m).astype(f32)
                ramp = jnp.clip(rel - (start + d), 0.0, 1.0)
                ty = last - ramp
                last = ramp
                for p in range(2):
                    term = jnp.where(here, near[8 * p : 8 * p + 8], far[8 * p : 8 * p + 8]) * ty
                    totals[p] = term if d == 0 else totals[p] + term
            res = totals[0] * w0_s[b, r, :] + totals[1] * w1_s[b, r, :]
            out.append(res if accs[g] is None else accs[g] + res)
        return tuple(out)

    def put(b, rows):
        rows = jnp.concatenate(rows, axis=0)
        accum[b] = rows
        out_ref[:, pl.ds(b * 128 if isinstance(b, int) else pl.multiple_of(b * 128, 128), 128)] = rows.astype(jnp.bfloat16)

    ahead = [pull(source_of(b), 0.0, FIRST) for b in range(1)]
    for b in range(blocks):
        if b + 1 < blocks:
            ahead.append(pull(source_of(b + 1), 0.0, FIRST))
        put(b, blend(b, ahead.pop(0), 0.0, FIRST, (None,) * GROUPS))
    bring.wait()

    @pl.when(num_m[0, blocks] > 0)
    def _():
        def again(b, _):
            def more(k, accs):
                start = (FIRST + MORE * k).astype(f32)
                return blend(b, pull(source_of(b), start, MORE), start, MORE, accs)

            @pl.when(num_m[0, b] > 0)
            def _():
                accs = tuple(accum[b, 8 * g : 8 * g + 8, :] for g in range(GROUPS))
                put(b, lax.fori_loop(0, num_m[0, b], more, accs))

            return 0

        lax.fori_loop(0, blocks, again, 0)


def render(first, count, fitted):
    vm = pl.BlockSpec(memory_space=pltpu.VMEM)
    return pl.pallas_call(
        render_kernel,
        out_shape=(
            jax.ShapeDtypeStruct((H, W), jnp.bfloat16),
            jax.ShapeDtypeStruct((6, VR, VC), jnp.float32),
        ),
        in_specs=[vm] * (2 + len(fitted)),
        out_specs=(vm, vm),
        scratch_shapes=[
            pltpu.VMEM((2, 2, H, W + 128), jnp.bfloat16),
            pltpu.VMEM((W // 128, H, 128), jnp.float32),
            pltpu.SMEM((8, 128), jnp.int32),
            pltpu.SemaphoreType.DMA,
        ],
        compiler_params=pltpu.CompilerParams(vmem_limit_bytes=16 << 20),
        name="render",
    )(first, count, *fitted)


def per_device(points, source, slab_first, slab_count):
    points, source = [pltpu.with_memory_space_constraint(x, pltpu.HBM) for x in (points, source)]
    return render(slab_first, slab_count, fit(points, source))


def solution(mesh):
    return jax.shard_map(
        per_device,
        mesh=mesh,
        in_specs=(
            P(None, ("sec", "ty")),
            P(("sec", "ty"), None),
            P(("sec", "ty")),
            P(("sec", "ty")),
        ),
        out_specs=(P(("sec", "ty"), None), P(None, ("sec", "ty"), None)),
        check_vma=False,
    )
```

```python
import math

import jax
import jax.numpy as jnp
from jax import lax
from jax.experimental import pallas as pl
from jax.experimental.pallas import tpu as pltpu
from jax.sharding import PartitionSpec as P

W = 2048
BH = 16
SP = 8
H = 32
K = 6
VR = 4
VC = 256


MESH = pl.DeviceIdType.MESH
RIDGE_TERM = 0.01


def solve_affine(moments, vertex_x, vertex_y):
    scale = 1.0 / moments[0]
    mean_px, mean_py, mean_qx, mean_qy = [m * scale for m in moments[1:5]]
    cov_xx = moments[5] * scale - mean_px * mean_px + RIDGE_TERM
    cov_xy = moments[6] * scale - mean_px * mean_py
    cov_yy = moments[7] * scale - mean_py * mean_py + RIDGE_TERM
    cross_xx = moments[8] * scale - mean_qx * mean_px
    cross_xy = moments[9] * scale - mean_qx * mean_py
    cross_yx = moments[10] * scale - mean_qy * mean_px
    cross_yy = moments[11] * scale - mean_qy * mean_py
    inverse = 1.0 / (cov_xx * cov_yy - cov_xy * cov_xy)
    lin_xx = (cross_xx * cov_yy - cross_xy * cov_xy) * inverse
    lin_xy = (cross_xy * cov_xx - cross_xx * cov_xy) * inverse
    lin_yx = (cross_yx * cov_yy - cross_yy * cov_xy) * inverse
    lin_yy = (cross_yy * cov_xx - cross_yx * cov_xy) * inverse
    delta_x = vertex_x - mean_px
    delta_y = vertex_y - mean_py
    shift_x = mean_qx + lin_xx * delta_x + lin_xy * delta_y - vertex_x
    shift_y = mean_qy + lin_yx * delta_x + lin_yy * delta_y - vertex_y
    return [lin_xx, lin_xy, lin_yx, lin_yy, shift_x, shift_y]


GROUPS = H // SP
FIRST = 10
UB = 16
UP = 4
MORE = 2
PER = 7


def pick(x, lanes):
    dims = lax.GatherDimensionNumbers(
        offset_dims=(), collapsed_slice_dims=(1,), start_index_map=(1,),
        operand_batching_dims=(0,), start_indices_batching_dims=(0,))
    return lax.gather(x, lanes[..., None], dims, slice_sizes=(1, 1),
                      mode=lax.GatherScatterMode.PROMISE_IN_BOUNDS)


def page_rows(rows_ref, to, there):
    lanes = lax.broadcasted_iota(jnp.int32, (H, 128), 1)
    zero = jnp.zeros((H, 128), jnp.bfloat16)
    prev = [zero, zero]
    for k in range(W // 128 + 1):
        now = zero
        if k < W // 128:
            now = rows_ref[:, 128 * k : 128 * k + 128]
            if there is not None:
                now = jnp.where(there, now, zero)
        for p, turn in enumerate((64, 63)):
            turned = pltpu.roll(now, turn, 1) if k < W // 128 else zero
            to[p, :, 128 * k : 128 * k + 128] = jnp.where(lanes < turn, prev[p], turned)
            prev[p] = turned


def positions(shifts, ext, num_ref, sp_s, low_s, far_s, ix_s, w0_s, w1_s):
    blocks = W // 128
    f32 = jnp.float32
    left, right = shifts[:, 0:128], shifts[:, 128:256]
    lane16 = lax.broadcasted_iota(jnp.int32, (16, 128), 1)
    ext[0] = jnp.where(lane16 < 1, left[:, 0:1], pltpu.roll(left, 1, 1))
    ext[1] = jnp.where(lane16 < 17, pltpu.roll(left, 17, 1), pltpu.roll(right, 17, 1))
    ext[2] = jnp.where(lane16 < 33, pltpu.roll(right, 33, 1), right[:, 127:128])

    sub = lax.broadcasted_iota(jnp.int32, (8, 128), 0)
    subf = sub.astype(f32)
    lane = lax.broadcasted_iota(jnp.int32, (8, 128), 1)
    wa = jnp.maximum(0.0, 1.0 - (subf + 4.0) * (1.0 / SP))
    wb = jnp.maximum(0.0, 1.0 - jnp.abs(subf - 4.0) * (1.0 / SP))
    wc = jnp.maximum(0.0, 1.0 - (12.0 - subf) * (1.0 / SP))
    wa, wb, wc = H * wa, H * wb, H * wc
    column = lane.astype(f32) + 64.0
    step = (lane + SP // 2) // SP
    part = ((lane + SP // 2) % SP).astype(f32) * (1.0 / SP)

    def prepare(b, spans):
        page = b // PER
        at = step + (b - page * PER) * (128 // SP)
        fine = []
        for half in range(2):
            held = ext[page, 8 * half : 8 * half + 8, :]
            near = pick(held, at)
            fine.append(near + part * (pick(held, at + 1) - near))
        fx, fy = fine
        most = None
        for g in range(GROUPS):
            dx = wa * fx[g : g + 1] + wb * fx[g + 1 : g + 2] + wc * fx[g + 2 : g + 3]
            dy = wa * fy[g : g + 1] + wb * fy[g + 1 : g + 2] + wc * fy[g + 2 : g + 3]
            sy = jnp.clip((subf + 8.0 * g) + dy, -33.0, 64.0)
            lx = jnp.clip(column + dx, -1.0, 256.0)
            base = jnp.clip(jnp.floor(lx), 0.0, 255.0)
            past = lx - base
            taps = [1.0 - jnp.abs(past), jnp.maximum(jnp.minimum(past, 255.0 - base), 0.0)]
            low = jnp.floor(jnp.min(sy, axis=1, keepdims=True))
            rel = sy - low
            most = rel if most is None else jnp.maximum(most, rel)
            r, tall = slice(8 * g, 8 * g + 8), slice(16 * g, 16 * g + 16)
            sp_s[b, r, :] = rel
            low_s[b, r, :] = jnp.broadcast_to(low, (8, 128))
            far_s[b, r, :] = base
            at = base.astype(jnp.int32)
            ix_s[b, tall, :] = jnp.concatenate([at, at], axis=0).astype(jnp.int16)
            taps = jnp.concatenate(taps, axis=0).astype(jnp.bfloat16).astype(f32)
            w0_s[b, r, :] = taps[0:8]
            w1_s[b, r, :] = taps[8:16]
        return jnp.where(lane == b, jnp.max(most, axis=1, keepdims=True), spans)

    spans = jnp.zeros((8, 128), f32)
    for b in range(blocks):
        spans = prepare(b, spans)
    rows = jnp.floor(jnp.max(spans, axis=0, keepdims=True)).astype(jnp.int32) + 2
    extra = (jnp.maximum(rows - FIRST, 0) + (MORE - 1)) // MORE
    extra = jnp.where(lane[0:1] == blocks, jnp.max(extra, axis=1, keepdims=True), extra)
    num_ref[...] = jnp.broadcast_to(extra, (8, 128))


OFFSETS = (1, -1, 2, -2)
FAR = 1e5
RATE = -2.0 * math.log2(math.e)
SKIP = 1e3


def halves(x):
    high = x.astype(jnp.bfloat16)
    return high, (x - high.astype(jnp.float32)).astype(jnp.bfloat16)


def fit_kernel(pts_ref, src_ref, fit_ref, num_ref, sp_s, low_s, far_s, ix_s, w0_s, w1_s, paged, wide,
               rows_s, ext, held, staged, mom, side, send_p, recv_p, send_s, recv_s, load):
    f32 = jnp.float32
    me = lax.axis_index("ty")
    n = lax.axis_size("ty")
    half = pts_ref.shape[1] // 2
    pairs = W // 256

    def exists(d):
        return (me + d >= 0) & (me + d < n)

    own_points = [
        pltpu.make_async_copy(pts_ref.at[:, pl.ds(c * half, half)], held.at[2, pl.ds(4 * c, 4)], load.at[c])
        for c in range(2)
    ]
    for c in own_points:
        c.start()
    own_rows = pltpu.make_async_copy(src_ref, rows_s, load.at[2])
    own_rows.start()
    barrier = pltpu.get_barrier_semaphore()
    for d in OFFSETS:
        @pl.when(exists(d))
        def _(d=d):
            pl.semaphore_signal(barrier, inc=1, device_id={"ty": me + d}, device_id_type=MESH)
    peers = sum(exists(d).astype(jnp.int32) for d in OFFSETS)

    def points_to(i, d):
        return pltpu.make_async_remote_copy(
            src_ref=held.at[2], dst_ref=held.at[2 - d], send_sem=send_p.at[i], recv_sem=recv_p.at[i],
            device_id={"ty": me + d}, device_id_type=MESH)

    def source_to(i, d):
        return pltpu.make_async_remote_copy(
            src_ref=src_ref, dst_ref=wide.at[i], send_sem=send_s.at[i], recv_sem=recv_s.at[i],
            device_id={"ty": me + d}, device_id_type=MESH)

    for c in own_points:
        c.wait()
    pl.semaphore_wait(barrier, peers)
    for i, d in enumerate(OFFSETS):
        @pl.when(exists(d))
        def _(i=i, d=d):
            points_to(i, d).start()
    for i, d in enumerate(OFFSETS[:2]):
        @pl.when(exists(d))
        def _(i=i, d=d):
            source_to(i, d).start()

    wide_lane = lax.broadcasted_iota(jnp.int32, (8, half + 128), 1) // 128
    wide_row = lax.broadcasted_iota(jnp.int32, (8, half + 128), 0) % 2
    centre = (me * H).astype(f32) + H / 2.0
    anchors = [
        jnp.where(wide_row == 0, ((2 * wide_lane + odd) * 256 + 128).astype(f32), centre) * (1.0 / H)
        for odd in range(2)
    ]
    spare = jnp.full((8, 128), FAR, f32)

    def stage(tile):
        data = held[2] if tile == 2 else jnp.where(exists(tile - 2), held[tile], FAR)
        row = jnp.concatenate([data, spare], axis=1) * (1.0 / H)
        staged[0, tile] = pltpu.roll(row, 32, 1) - anchors[0]
        staged[1, tile] = pltpu.roll(row, half + 96, 1) - anchors[1]

    e = lax.broadcasted_iota(jnp.int32, (8, 128), 0)
    vy = (((e - 1) * SP + SP // 2) - H // 2).astype(f32) * (1.0 / H)
    vy_of = {1: jnp.where(e == 5, SKIP, vy), 2: vy, 3: jnp.where(e == 0, SKIP, vy)}
    lone = {0: (-SP // 2 - H // 2) / H, 4: (4 * SP + SP // 2 - H // 2) / H}
    lane32 = lax.broadcasted_iota(jnp.int32, (32, 128), 1)
    vert32 = lax.broadcasted_iota(jnp.int32, (32, 128), 0)
    near = jnp.abs(lane32 // 32 - 1 - vert32 // 16) <= 1
    vx = jnp.where(near, (vert32 * SP + SP // 2 - 128).astype(f32) * (1.0 / H), SKIP)

    def bell(gap):
        return jnp.exp2((gap * gap) * RATE)

    def rows_of(k, odd, tile, c):
        at = pl.ds(pl.multiple_of(k * 128, 128), 128)
        return [jnp.broadcast_to(staged[odd, tile, 4 * c + i : 4 * c + i + 1, at], (8, 128)) for i in range(4)]

    def across(px):
        gap = jnp.concatenate([px - vx[8 * g : 8 * g + 8] for g in range(4)], axis=0)
        return jnp.concatenate(halves(bell(gap)), axis=0)

    def contract(parts, weights):
        return lax.dot_general(
            jnp.concatenate(parts, axis=1), jnp.concatenate(weights, axis=1),
            (((1,), (1,)), ((), ())), preferred_element_type=f32)

    def dense(k, odd, tiles):
        parts, weights = [], []
        for tile in tiles:
            for c in range(2):
                px, py, qx, qy = rows_of(k, odd, tile, c)
                weights.append(across(px))
                w = bell(py - vy_of[tile])
                wpx = w * px
                wpy = w * py
                feats = jnp.concatenate(
                    [w, wpx, wpy, w * qx, w * qy, wpx * px, wpx * py, wpy * py,
                     wpx * qx, wpy * qx, wpx * qy, wpy * qy], axis=0)
                parts.append(jnp.concatenate(halves(feats), axis=0))
        got = contract(parts, weights)
        got = got[0:96] + got[96:192]
        return got[:, 0:32] + got[:, 32:64]

    def single(k, odd, tile):
        parts, weights = [], []
        for c in range(2):
            px, py, qx, qy = rows_of(k, odd, tile, c)
            weights.append(across(px))
            w = bell(py - lone[tile])
            a1 = jnp.where(e == 0, 1.0, jnp.where((e == 2) | (e == 7), py, jnp.where(e == 3, qx, jnp.where(e == 4, qy, px))))
            b1 = jnp.where(e < 5, 1.0, jnp.where(e == 5, px, py))
            a2 = jnp.where(e % 2 == 0, px, py)
            b2 = jnp.where(e < 2, qx, qy)
            feats = jnp.concatenate([w * a1 * b1, w * a2 * b2], axis=0)
            parts.append(jnp.concatenate(halves(feats), axis=0))
        got = contract(parts, weights)
        got = got[0:16] + got[16:32]
        return got[:, 0:32] + got[:, 32:64]

    def own_group(k, _):
        for odd in range(2):
            mom[2 * k + odd] = dense(k, odd, (2,))
        return 0

    def next_group(k, _):
        for odd in range(2):
            mom[2 * k + odd] += dense(k, odd, (1, 3))
        return 0

    def last_group(k, _):
        for odd in range(2):
            for s, tile in enumerate((0, 4)):
                side[s, 2 * k + odd] = single(k, odd, tile)
        return 0

    def arrive(which):
        for i in which:
            @pl.when(exists(-OFFSETS[i]))
            def _(i=i):
                points_to(i, OFFSETS[i]).wait_recv()
        for i in which:
            stage(2 - OFFSETS[i])

    stage(2)
    lax.fori_loop(0, pairs // 2, own_group, 0, unroll=4)
    own_rows.wait()
    page_rows(rows_s, paged, None)
    arrive((0, 1))
    lax.fori_loop(0, pairs // 2, next_group, 0, unroll=4)
    arrive((2, 3))
    lax.fori_loop(0, pairs // 2, last_group, 0, unroll=4)

    ew = lax.broadcasted_iota(jnp.int32, (8, VC), 0)
    jw = lax.broadcasted_iota(jnp.int32, (8, VC), 1)
    vertex_y = (((ew - 1) * SP + SP // 2) - H // 2).astype(f32) * (1.0 / H)
    vertex_x = ((jw % 32) * SP + SP // 2 - 128).astype(f32) * (1.0 / H)
    safe = ew < 6
    sides = [jnp.concatenate([side[s, g] for g in range(pairs)], axis=1) for s in range(2)]
    moments = []
    for f in range(12):
        m = jnp.concatenate([mom[g, 8 * f : 8 * f + 8, :] for g in range(pairs)], axis=1)
        m = m + jnp.where(ew == 0, sides[0][f : f + 1], jnp.where(ew == 5, sides[1][f : f + 1], 0.0))
        moments.append(m)
    moments[0] = jnp.where(safe, moments[0], 1.0)
    solved = solve_affine(moments, vertex_x, vertex_y)
    for f in range(6):
        x = solved[f]
        if f >= 4:
            x = jnp.where((ew == 0) & (me == 0), x[1:2], x)
            x = jnp.where((ew == 5) & (me == n - 1), x[4:5], x)
            x = jnp.where(safe, x, 0.0)
        fit_ref[8 * f : 8 * f + 8, :] = x
        solved[f] = x
    positions(jnp.concatenate(solved[4:6], axis=0), ext, num_ref, sp_s, low_s, far_s, ix_s, w0_s, w1_s)

    for i, d in enumerate(OFFSETS[:2]):
        @pl.when(exists(-d))
        def _(i=i, d=d):
            source_to(i, d).wait_recv()
    for i, d in enumerate(OFFSETS):
        @pl.when(exists(d))
        def _(i=i, d=d):
            points_to(i, d).wait_send()
    for i, d in enumerate(OFFSETS[:2]):
        @pl.when(exists(d))
        def _(i=i, d=d):
            source_to(i, d).wait_send()


def fit(points, source):
    size = points.shape[1]
    blocks = W // 128
    per = lambda d: pltpu.VMEM((blocks, H, 128), d)
    vm = pl.BlockSpec(memory_space=pltpu.VMEM)
    return pl.pallas_call(
        fit_kernel,
        out_shape=(
            pltpu.VMEM((48, VC), jnp.float32),
            pltpu.VMEM((8, 128), jnp.int32),
            per(jnp.float32), per(jnp.float32), per(jnp.float32),
            pltpu.VMEM((blocks, 2 * H, 128), jnp.int16),
            per(jnp.float32), per(jnp.float32),
            pltpu.VMEM((2, H, W + 128), jnp.bfloat16),
            pltpu.VMEM((2, H, W), jnp.bfloat16),
        ),
        in_specs=[pl.BlockSpec(memory_space=pltpu.HBM)] * 2,
        out_specs=(vm,) * 10,
        scratch_shapes=[
            pltpu.VMEM((H, W), jnp.bfloat16),
            pltpu.VMEM((-(-blocks // PER), 16, 128), jnp.float32),
            pltpu.VMEM((5, 8, size // 2), jnp.float32),
            pltpu.VMEM((2, 5, 8, size // 2 + 128), jnp.float32),
            pltpu.VMEM((W // 256, 96, 32), jnp.float32),
            pltpu.VMEM((2, W // 256, 16, 32), jnp.float32),
            pltpu.SemaphoreType.DMA((4,)),
            pltpu.SemaphoreType.DMA((4,)),
            pltpu.SemaphoreType.DMA((2,)),
            pltpu.SemaphoreType.DMA((2,)),
            pltpu.SemaphoreType.DMA((3,)),
        ],
        compiler_params=pltpu.CompilerParams(collective_id=0, has_side_effects=True, vmem_limit_bytes=8 << 20),
        name="fit",
    )(points, source)


def render_kernel(first_ref, count_ref, fit_ref, num_ref, sp_s, low_s, far_s, ix_s, w0_s, w1_s, paged, wide_ref,
                  out_ref, aff_ref, halo, accum, num_m, sem):
    blocks = W // 128
    tile = lax.axis_index("ty")
    n = lax.axis_size("ty")
    f32 = jnp.float32
    bring = pltpu.make_async_copy(num_ref, num_m, sem)
    bring.start()
    for f in range(6):
        aff_ref[f] = fit_ref[8 * f + 1 : 8 * f + 5, :]

    page_rows(wide_ref.at[0], halo.at[0], tile > 0)
    page_rows(wide_ref.at[1], halo.at[1], tile < n - 1)
    slot = lax.broadcasted_iota(jnp.int32, (8, 3 * H), 1)
    first = jnp.broadcast_to(first_ref[...].reshape(1, 1), slot.shape) * BH - tile * H + H
    last = first + jnp.broadcast_to(count_ref[...].reshape(1, 1), slot.shape) * BH
    slot = jnp.where((slot >= first) & (slot < last), (slot - H).astype(f32), -1e6)

    def source_of(b):
        cols = pl.ds(b * 128 if isinstance(b, int) else pl.multiple_of(b * 128, 128), 256)
        window = [
            jnp.concatenate([halo[0, p, :, cols], paged[p, :, cols], halo[1, p, :, cols]], axis=0) for p in range(2)]
        lows = [slot - low_s[b, 8 * g : 8 * g + 8, :][:, : 3 * H] for g in range(GROUPS)]
        return window, lows

    def pull(held, start, size):
        window, lows = held
        onehot = jnp.concatenate(
            [jnp.where(lows[g] == start + d, 1.0, 0.0) for g in range(GROUPS) for d in range(size)], axis=0)
        onehot = onehot.astype(jnp.bfloat16)
        return [jnp.dot(onehot, w, preferred_element_type=f32) for w in window]

    def blend(b, got, start, size, accs):
        out = []
        for g in range(GROUPS):
            r = slice(8 * g, 8 * g + 8)
            lanes_at = ix_s[b, 16 * g : 16 * g + 16, :]
            m = lanes_at & 127
            here = far_s[b, r, :] < 128.0
            rel = sp_s[b, r, :]
            totals = [None, None]
            last = jnp.clip(rel - (start - 1.0), 0.0, 1.0)
            for d in range(size):
                at = slice(8 * (g * size + d), 8 * (g * size + d) + 8)
                near, far = [
                    jnp.concatenate([tap[at, side] for tap in got], axis=0).astype(jnp.bfloat16)
                    for side in (slice(0, 128), slice(128, 256))
                ]
                near, far = pick(near, m).astype(f32), pick(far, m).astype(f32)
                ramp = jnp.clip(rel - (start + d), 0.0, 1.0)
                ty = last - ramp
                last = ramp
                for p in range(2):
                    term = jnp.where(here, near[8 * p : 8 * p + 8], far[8 * p : 8 * p + 8]) * ty
                    totals[p] = term if d == 0 else totals[p] + term
            res = totals[0] * w0_s[b, r, :] + totals[1] * w1_s[b, r, :]
            out.append(res if accs[g] is None else accs[g] + res)
        return tuple(out)

    def put(b, rows):
        rows = jnp.concatenate(rows, axis=0)
        accum[b] = rows
        out_ref[:, pl.ds(b * 128 if isinstance(b, int) else pl.multiple_of(b * 128, 128), 128)] = rows.astype(jnp.bfloat16)

    ahead = [pull(source_of(b), 0.0, FIRST) for b in range(1)]
    for b in range(blocks):
        if b + 1 < blocks:
            ahead.append(pull(source_of(b + 1), 0.0, FIRST))
        put(b, blend(b, ahead.pop(0), 0.0, FIRST, (None,) * GROUPS))
    bring.wait()

    @pl.when(num_m[0, blocks] > 0)
    def _():
        def again(b, _):
            def more(k, accs):
                start = (FIRST + MORE * k).astype(f32)
                return blend(b, pull(source_of(b), start, MORE), start, MORE, accs)

            @pl.when(num_m[0, b] > 0)
            def _():
                accs = tuple(accum[b, 8 * g : 8 * g + 8, :] for g in range(GROUPS))
                put(b, lax.fori_loop(0, num_m[0, b], more, accs))

            return 0

        lax.fori_loop(0, blocks, again, 0)


def render(first, count, fitted):
    vm = pl.BlockSpec(memory_space=pltpu.VMEM)
    return pl.pallas_call(
        render_kernel,
        out_shape=(
            jax.ShapeDtypeStruct((H, W), jnp.bfloat16),
            jax.ShapeDtypeStruct((6, VR, VC), jnp.float32),
        ),
        in_specs=[vm] * (2 + len(fitted)),
        out_specs=(vm, vm),
        scratch_shapes=[
            pltpu.VMEM((2, 2, H, W + 128), jnp.bfloat16),
            pltpu.VMEM((W // 128, H, 128), jnp.float32),
            pltpu.SMEM((8, 128), jnp.int32),
            pltpu.SemaphoreType.DMA,
        ],
        compiler_params=pltpu.CompilerParams(vmem_limit_bytes=16 << 20),
        name="render",
    )(first, count, *fitted)


def per_device(points, source, slab_first, slab_count):
    points, source = [pltpu.with_memory_space_constraint(x, pltpu.HBM) for x in (points, source)]
    return render(slab_first, slab_count, fit(points, source))


def solution(mesh):
    return jax.shard_map(
        per_device,
        mesh=mesh,
        in_specs=(
            P(None, ("sec", "ty")),
            P(("sec", "ty"), None),
            P(("sec", "ty")),
            P(("sec", "ty")),
        ),
        out_specs=(P(("sec", "ty"), None), P(None, ("sec", "ty"), None)),
        check_vma=False,
    )
```

```python
import math

import jax
import jax.numpy as jnp
from jax import lax
from jax.experimental import pallas as pl
from jax.experimental.pallas import tpu as pltpu
from jax.sharding import PartitionSpec as P

W = 2048
BH = 16
SP = 8
H = 32
K = 6
VR = 4
VC = 256


MESH = pl.DeviceIdType.MESH
RIDGE_TERM = 0.01


def solve_affine(moments, vertex_x, vertex_y):
    scale = 1.0 / moments[0]
    mean_px, mean_py, mean_qx, mean_qy = [m * scale for m in moments[1:5]]
    cov_xx = moments[5] * scale - mean_px * mean_px + RIDGE_TERM
    cov_xy = moments[6] * scale - mean_px * mean_py
    cov_yy = moments[7] * scale - mean_py * mean_py + RIDGE_TERM
    cross_xx = moments[8] * scale - mean_qx * mean_px
    cross_xy = moments[9] * scale - mean_qx * mean_py
    cross_yx = moments[10] * scale - mean_qy * mean_px
    cross_yy = moments[11] * scale - mean_qy * mean_py
    inverse = 1.0 / (cov_xx * cov_yy - cov_xy * cov_xy)
    lin_xx = (cross_xx * cov_yy - cross_xy * cov_xy) * inverse
    lin_xy = (cross_xy * cov_xx - cross_xx * cov_xy) * inverse
    lin_yx = (cross_yx * cov_yy - cross_yy * cov_xy) * inverse
    lin_yy = (cross_yy * cov_xx - cross_yx * cov_xy) * inverse
    delta_x = vertex_x - mean_px
    delta_y = vertex_y - mean_py
    shift_x = mean_qx + lin_xx * delta_x + lin_xy * delta_y - vertex_x
    shift_y = mean_qy + lin_yx * delta_x + lin_yy * delta_y - vertex_y
    return [lin_xx, lin_xy, lin_yx, lin_yy, shift_x, shift_y]


GROUPS = H // SP
FIRST = 9
UB = 16
UP = 4
MORE = 1
PER = 7


def pick(x, lanes):
    dims = lax.GatherDimensionNumbers(
        offset_dims=(), collapsed_slice_dims=(1,), start_index_map=(1,),
        operand_batching_dims=(0,), start_indices_batching_dims=(0,))
    return lax.gather(x, lanes[..., None], dims, slice_sizes=(1, 1),
                      mode=lax.GatherScatterMode.PROMISE_IN_BOUNDS)


def page_rows(rows_ref, to, there):
    lanes = lax.broadcasted_iota(jnp.int32, (H, 128), 1)
    zero = jnp.zeros((H, 128), jnp.bfloat16)
    prev = [zero, zero]
    for k in range(W // 128 + 1):
        now = zero
        if k < W // 128:
            now = rows_ref[:, 128 * k : 128 * k + 128]
            if there is not None:
                now = jnp.where(there, now, zero)
        for p, turn in enumerate((64, 63)):
            turned = pltpu.roll(now, turn, 1) if k < W // 128 else zero
            to[p, :, 128 * k : 128 * k + 128] = jnp.where(lanes < turn, prev[p], turned)
            prev[p] = turned


def positions(shifts, ext, num_ref, sp_s, low_s, far_s, ix_s, w0_s, w1_s):
    blocks = W // 128
    f32 = jnp.float32
    left, right = shifts[:, 0:128], shifts[:, 128:256]
    lane16 = lax.broadcasted_iota(jnp.int32, (16, 128), 1)
    ext[0] = jnp.where(lane16 < 1, left[:, 0:1], pltpu.roll(left, 1, 1))
    ext[1] = jnp.where(lane16 < 17, pltpu.roll(left, 17, 1), pltpu.roll(right, 17, 1))
    ext[2] = jnp.where(lane16 < 33, pltpu.roll(right, 33, 1), right[:, 127:128])

    sub = lax.broadcasted_iota(jnp.int32, (8, 128), 0)
    subf = sub.astype(f32)
    lane = lax.broadcasted_iota(jnp.int32, (8, 128), 1)
    wa = jnp.maximum(0.0, 1.0 - (subf + 4.0) * (1.0 / SP))
    wb = jnp.maximum(0.0, 1.0 - jnp.abs(subf - 4.0) * (1.0 / SP))
    wc = jnp.maximum(0.0, 1.0 - (12.0 - subf) * (1.0 / SP))
    wa, wb, wc = H * wa, H * wb, H * wc
    column = lane.astype(f32) + 64.0
    step = (lane + SP // 2) // SP
    part = ((lane + SP // 2) % SP).astype(f32) * (1.0 / SP)

    def prepare(b, spans):
        page = b // PER
        at = step + (b - page * PER) * (128 // SP)
        fine = []
        for half in range(2):
            held = ext[page, 8 * half : 8 * half + 8, :]
            near = pick(held, at)
            fine.append(near + part * (pick(held, at + 1) - near))
        fx, fy = fine
        most = None
        for g in range(GROUPS):
            dx = wa * fx[g : g + 1] + wb * fx[g + 1 : g + 2] + wc * fx[g + 2 : g + 3]
            dy = wa * fy[g : g + 1] + wb * fy[g + 1 : g + 2] + wc * fy[g + 2 : g + 3]
            sy = jnp.clip((subf + 8.0 * g) + dy, -33.0, 64.0)
            lx = jnp.clip(column + dx, -1.0, 256.0)
            base = jnp.clip(jnp.floor(lx), 0.0, 255.0)
            past = lx - base
            taps = [1.0 - jnp.abs(past), jnp.maximum(jnp.minimum(past, 255.0 - base), 0.0)]
            low = jnp.floor(jnp.min(sy, axis=1, keepdims=True))
            rel = sy - low
            most = rel if most is None else jnp.maximum(most, rel)
            r, tall = slice(8 * g, 8 * g + 8), slice(16 * g, 16 * g + 16)
            sp_s[b, r, :] = rel
            low_s[b, r, :] = jnp.broadcast_to(low, (8, 128))
            far_s[b, r, :] = base
            at = base.astype(jnp.int32)
            ix_s[b, tall, :] = jnp.concatenate([at, at], axis=0).astype(jnp.int16)
            taps = jnp.concatenate(taps, axis=0).astype(jnp.bfloat16).astype(f32)
            w0_s[b, r, :] = taps[0:8]
            w1_s[b, r, :] = taps[8:16]
        return jnp.where(lane == b, jnp.max(most, axis=1, keepdims=True), spans)

    spans = jnp.zeros((8, 128), f32)
    for b in range(blocks):
        spans = prepare(b, spans)
    rows = jnp.floor(jnp.max(spans, axis=0, keepdims=True)).astype(jnp.int32) + 2
    extra = (jnp.maximum(rows - FIRST, 0) + (MORE - 1)) // MORE
    extra = jnp.where(lane[0:1] == blocks, jnp.max(extra, axis=1, keepdims=True), extra)
    num_ref[...] = jnp.broadcast_to(extra, (8, 128))


OFFSETS = (1, -1, 2, -2)
FAR = 1e5
RATE = -2.0 * math.log2(math.e)
SKIP = 1e3


def halves(x):
    high = x.astype(jnp.bfloat16)
    return high, (x - high.astype(jnp.float32)).astype(jnp.bfloat16)


def fit_kernel(pts_ref, src_ref, fit_ref, num_ref, sp_s, low_s, far_s, ix_s, w0_s, w1_s, paged, wide,
               rows_s, ext, held, staged, mom, side, send_p, recv_p, send_s, recv_s, load):
    f32 = jnp.float32
    me = lax.axis_index("ty")
    n = lax.axis_size("ty")
    half = pts_ref.shape[1] // 2
    pairs = W // 256

    def exists(d):
        return (me + d >= 0) & (me + d < n)

    own_points = [
        pltpu.make_async_copy(pts_ref.at[:, pl.ds(c * half, half)], held.at[2, pl.ds(4 * c, 4)], load.at[c])
        for c in range(2)
    ]
    for c in own_points:
        c.start()
    own_rows = pltpu.make_async_copy(src_ref, rows_s, load.at[2])
    own_rows.start()
    barrier = pltpu.get_barrier_semaphore()
    for d in OFFSETS:
        @pl.when(exists(d))
        def _(d=d):
            pl.semaphore_signal(barrier, inc=1, device_id={"ty": me + d}, device_id_type=MESH)
    peers = sum(exists(d).astype(jnp.int32) for d in OFFSETS)

    def points_to(i, d):
        return pltpu.make_async_remote_copy(
            src_ref=held.at[2], dst_ref=held.at[2 - d], send_sem=send_p.at[i], recv_sem=recv_p.at[i],
            device_id={"ty": me + d}, device_id_type=MESH)

    def source_to(i, d):
        return pltpu.make_async_remote_copy(
            src_ref=src_ref, dst_ref=wide.at[i], send_sem=send_s.at[i], recv_sem=recv_s.at[i],
            device_id={"ty": me + d}, device_id_type=MESH)

    for c in own_points:
        c.wait()
    pl.semaphore_wait(barrier, peers)
    for i, d in enumerate(OFFSETS):
        @pl.when(exists(d))
        def _(i=i, d=d):
            points_to(i, d).start()
    for i, d in enumerate(OFFSETS[:2]):
        @pl.when(exists(d))
        def _(i=i, d=d):
            source_to(i, d).start()

    wide_lane = lax.broadcasted_iota(jnp.int32, (8, half + 128), 1) // 128
    wide_row = lax.broadcasted_iota(jnp.int32, (8, half + 128), 0) % 2
    centre = (me * H).astype(f32) + H / 2.0
    anchors = [
        jnp.where(wide_row == 0, ((2 * wide_lane + odd) * 256 + 128).astype(f32), centre) * (1.0 / H)
        for odd in range(2)
    ]
    spare = jnp.full((8, 128), FAR, f32)

    def stage(tile):
        data = held[2] if tile == 2 else jnp.where(exists(tile - 2), held[tile], FAR)
        row = jnp.concatenate([data, spare], axis=1) * (1.0 / H)
        staged[0, tile] = pltpu.roll(row, 32, 1) - anchors[0]
        staged[1, tile] = pltpu.roll(row, half + 96, 1) - anchors[1]

    e = lax.broadcasted_iota(jnp.int32, (8, 128), 0)
    vy = (((e - 1) * SP + SP // 2) - H // 2).astype(f32) * (1.0 / H)
    vy_of = {1: jnp.where(e == 5, SKIP, vy), 2: vy, 3: jnp.where(e == 0, SKIP, vy)}
    lone = {0: (-SP // 2 - H // 2) / H, 4: (4 * SP + SP // 2 - H // 2) / H}
    lane32 = lax.broadcasted_iota(jnp.int32, (32, 128), 1)
    vert32 = lax.broadcasted_iota(jnp.int32, (32, 128), 0)
    near = jnp.abs(lane32 // 32 - 1 - vert32 // 16) <= 1
    vx = jnp.where(near, (vert32 * SP + SP // 2 - 128).astype(f32) * (1.0 / H), SKIP)

    def bell(gap):
        return jnp.exp2((gap * gap) * RATE)

    def rows_of(k, odd, tile, c):
        at = pl.ds(pl.multiple_of(k * 128, 128), 128)
        return [jnp.broadcast_to(staged[odd, tile, 4 * c + i : 4 * c + i + 1, at], (8, 128)) for i in range(4)]

    def across(px):
        gap = jnp.concatenate([px - vx[8 * g : 8 * g + 8] for g in range(4)], axis=0)
        return jnp.concatenate(halves(bell(gap)), axis=0)

    def contract(parts, weights):
        return lax.dot_general(
            jnp.concatenate(parts, axis=1), jnp.concatenate(weights, axis=1),
            (((1,), (1,)), ((), ())), preferred_element_type=f32)

    def dense(k, odd, tiles):
        parts, weights = [], []
        for tile in tiles:
            for c in range(2):
                px, py, qx, qy = rows_of(k, odd, tile, c)
                weights.append(across(px))
                w = bell(py - vy_of[tile])
                wpx = w * px
                wpy = w * py
                feats = jnp.concatenate(
                    [w, wpx, wpy, w * qx, w * qy, wpx * px, wpx * py, wpy * py,
                     wpx * qx, wpy * qx, wpx * qy, wpy * qy], axis=0)
                parts.append(jnp.concatenate(halves(feats), axis=0))
        got = contract(parts, weights)
        got = got[0:96] + got[96:192]
        return got[:, 0:32] + got[:, 32:64]

    def single(k, odd, tile):
        parts, weights = [], []
        for c in range(2):
            px, py, qx, qy = rows_of(k, odd, tile, c)
            weights.append(across(px))
            w = bell(py - lone[tile])
            a1 = jnp.where(e == 0, 1.0, jnp.where((e == 2) | (e == 7), py, jnp.where(e == 3, qx, jnp.where(e == 4, qy, px))))
            b1 = jnp.where(e < 5, 1.0, jnp.where(e == 5, px, py))
            a2 = jnp.where(e % 2 == 0, px, py)
            b2 = jnp.where(e < 2, qx, qy)
            feats = jnp.concatenate([w * a1 * b1, w * a2 * b2], axis=0)
            parts.append(jnp.concatenate(halves(feats), axis=0))
        got = contract(parts, weights)
        got = got[0:16] + got[16:32]
        return got[:, 0:32] + got[:, 32:64]

    def own_group(k, _):
        for odd in range(2):
            mom[2 * k + odd] = dense(k, odd, (2,))
        return 0

    def next_group(k, _):
        for odd in range(2):
            mom[2 * k + odd] += dense(k, odd, (1, 3))
        return 0

    def last_group(k, _):
        for odd in range(2):
            for s, tile in enumerate((0, 4)):
                side[s, 2 * k + odd] = single(k, odd, tile)
        return 0

    def arrive(which):
        for i in which:
            @pl.when(exists(-OFFSETS[i]))
            def _(i=i):
                points_to(i, OFFSETS[i]).wait_recv()
        for i in which:
            stage(2 - OFFSETS[i])

    stage(2)
    lax.fori_loop(0, pairs // 2, own_group, 0, unroll=4)
    own_rows.wait()
    page_rows(rows_s, paged, None)
    arrive((0, 1))
    lax.fori_loop(0, pairs // 2, next_group, 0, unroll=4)
    arrive((2, 3))
    lax.fori_loop(0, pairs // 2, last_group, 0, unroll=4)

    ew = lax.broadcasted_iota(jnp.int32, (8, VC), 0)
    jw = lax.broadcasted_iota(jnp.int32, (8, VC), 1)
    vertex_y = (((ew - 1) * SP + SP // 2) - H // 2).astype(f32) * (1.0 / H)
    vertex_x = ((jw % 32) * SP + SP // 2 - 128).astype(f32) * (1.0 / H)
    safe = ew < 6
    sides = [jnp.concatenate([side[s, g] for g in range(pairs)], axis=1) for s in range(2)]
    moments = []
    for f in range(12):
        m = jnp.concatenate([mom[g, 8 * f : 8 * f + 8, :] for g in range(pairs)], axis=1)
        m = m + jnp.where(ew == 0, sides[0][f : f + 1], jnp.where(ew == 5, sides[1][f : f + 1], 0.0))
        moments.append(m)
    moments[0] = jnp.where(safe, moments[0], 1.0)
    solved = solve_affine(moments, vertex_x, vertex_y)
    for f in range(6):
        x = solved[f]
        if f >= 4:
            x = jnp.where((ew == 0) & (me == 0), x[1:2], x)
            x = jnp.where((ew == 5) & (me == n - 1), x[4:5], x)
            x = jnp.where(safe, x, 0.0)
        fit_ref[8 * f : 8 * f + 8, :] = x
        solved[f] = x
    positions(jnp.concatenate(solved[4:6], axis=0), ext, num_ref, sp_s, low_s, far_s, ix_s, w0_s, w1_s)

    for i, d in enumerate(OFFSETS[:2]):
        @pl.when(exists(-d))
        def _(i=i, d=d):
            source_to(i, d).wait_recv()
    for i, d in enumerate(OFFSETS):
        @pl.when(exists(d))
        def _(i=i, d=d):
            points_to(i, d).wait_send()
    for i, d in enumerate(OFFSETS[:2]):
        @pl.when(exists(d))
        def _(i=i, d=d):
            source_to(i, d).wait_send()


def fit(points, source):
    size = points.shape[1]
    blocks = W // 128
    per = lambda d: pltpu.VMEM((blocks, H, 128), d)
    vm = pl.BlockSpec(memory_space=pltpu.VMEM)
    return pl.pallas_call(
        fit_kernel,
        out_shape=(
            pltpu.VMEM((48, VC), jnp.float32),
            pltpu.VMEM((8, 128), jnp.int32),
            per(jnp.float32), per(jnp.float32), per(jnp.float32),
            pltpu.VMEM((blocks, 2 * H, 128), jnp.int16),
            per(jnp.float32), per(jnp.float32),
            pltpu.VMEM((2, H, W + 128), jnp.bfloat16),
            pltpu.VMEM((2, H, W), jnp.bfloat16),
        ),
        in_specs=[pl.BlockSpec(memory_space=pltpu.HBM)] * 2,
        out_specs=(vm,) * 10,
        scratch_shapes=[
            pltpu.VMEM((H, W), jnp.bfloat16),
            pltpu.VMEM((-(-blocks // PER), 16, 128), jnp.float32),
            pltpu.VMEM((5, 8, size // 2), jnp.float32),
            pltpu.VMEM((2, 5, 8, size // 2 + 128), jnp.float32),
            pltpu.VMEM((W // 256, 96, 32), jnp.float32),
            pltpu.VMEM((2, W // 256, 16, 32), jnp.float32),
            pltpu.SemaphoreType.DMA((4,)),
            pltpu.SemaphoreType.DMA((4,)),
            pltpu.SemaphoreType.DMA((2,)),
            pltpu.SemaphoreType.DMA((2,)),
            pltpu.SemaphoreType.DMA((3,)),
        ],
        compiler_params=pltpu.CompilerParams(collective_id=0, has_side_effects=True, vmem_limit_bytes=8 << 20),
        name="fit",
    )(points, source)


def render_kernel(first_ref, count_ref, fit_ref, num_ref, sp_s, low_s, far_s, ix_s, w0_s, w1_s, paged, wide_ref,
                  out_ref, aff_ref, halo, accum, num_m, sem):
    blocks = W // 128
    tile = lax.axis_index("ty")
    n = lax.axis_size("ty")
    f32 = jnp.float32
    bring = pltpu.make_async_copy(num_ref, num_m, sem)
    bring.start()
    for f in range(6):
        aff_ref[f] = fit_ref[8 * f + 1 : 8 * f + 5, :]

    page_rows(wide_ref.at[0], halo.at[0], tile > 0)
    page_rows(wide_ref.at[1], halo.at[1], tile < n - 1)
    slot = lax.broadcasted_iota(jnp.int32, (8, 3 * H), 1)
    first = jnp.broadcast_to(first_ref[...].reshape(1, 1), slot.shape) * BH - tile * H + H
    last = first + jnp.broadcast_to(count_ref[...].reshape(1, 1), slot.shape) * BH
    slot = jnp.where((slot >= first) & (slot < last), (slot - H).astype(f32), -1e6)

    def source_of(b):
        cols = pl.ds(b * 128 if isinstance(b, int) else pl.multiple_of(b * 128, 128), 256)
        window = [
            jnp.concatenate([halo[0, p, :, cols], paged[p, :, cols], halo[1, p, :, cols]], axis=0) for p in range(2)]
        lows = [slot - low_s[b, 8 * g : 8 * g + 8, :][:, : 3 * H] for g in range(GROUPS)]
        return window, lows

    def pull(held, start, size):
        window, lows = held
        onehot = jnp.concatenate(
            [jnp.where(lows[g] == start + d, 1.0, 0.0) for g in range(GROUPS) for d in range(size)], axis=0)
        onehot = onehot.astype(jnp.bfloat16)
        return [jnp.dot(onehot, w, preferred_element_type=f32) for w in window]

    def blend(b, got, start, size, accs):
        out = []
        for g in range(GROUPS):
            r = slice(8 * g, 8 * g + 8)
            lanes_at = ix_s[b, 16 * g : 16 * g + 16, :]
            m = lanes_at & 127
            here = far_s[b, r, :] < 128.0
            rel = sp_s[b, r, :]
            totals = [None, None]
            last = jnp.clip(rel - (start - 1.0), 0.0, 1.0)
            for d in range(size):
                at = slice(8 * (g * size + d), 8 * (g * size + d) + 8)
                near, far = [
                    jnp.concatenate([tap[at, side] for tap in got], axis=0).astype(jnp.bfloat16)
                    for side in (slice(0, 128), slice(128, 256))
                ]
                near, far = pick(near, m).astype(f32), pick(far, m).astype(f32)
                ramp = jnp.clip(rel - (start + d), 0.0, 1.0)
                ty = last - ramp
                last = ramp
                for p in range(2):
                    term = jnp.where(here, near[8 * p : 8 * p + 8], far[8 * p : 8 * p + 8]) * ty
                    totals[p] = term if d == 0 else totals[p] + term
            res = totals[0] * w0_s[b, r, :] + totals[1] * w1_s[b, r, :]
            out.append(res if accs[g] is None else accs[g] + res)
        return tuple(out)

    def put(b, rows):
        rows = jnp.concatenate(rows, axis=0)
        accum[b] = rows
        out_ref[:, pl.ds(b * 128 if isinstance(b, int) else pl.multiple_of(b * 128, 128), 128)] = rows.astype(jnp.bfloat16)

    ahead = [pull(source_of(b), 0.0, FIRST) for b in range(1)]
    for b in range(blocks):
        if b + 1 < blocks:
            ahead.append(pull(source_of(b + 1), 0.0, FIRST))
        put(b, blend(b, ahead.pop(0), 0.0, FIRST, (None,) * GROUPS))
    bring.wait()

    @pl.when(num_m[0, blocks] > 0)
    def _():
        def again(b, _):
            def more(k, accs):
                start = (FIRST + MORE * k).astype(f32)
                return blend(b, pull(source_of(b), start, MORE), start, MORE, accs)

            @pl.when(num_m[0, b] > 0)
            def _():
                accs = tuple(accum[b, 8 * g : 8 * g + 8, :] for g in range(GROUPS))
                put(b, lax.fori_loop(0, num_m[0, b], more, accs))

            return 0

        lax.fori_loop(0, blocks, again, 0)


def render(first, count, fitted):
    vm = pl.BlockSpec(memory_space=pltpu.VMEM)
    return pl.pallas_call(
        render_kernel,
        out_shape=(
            jax.ShapeDtypeStruct((H, W), jnp.bfloat16),
            jax.ShapeDtypeStruct((6, VR, VC), jnp.float32),
        ),
        in_specs=[vm] * (2 + len(fitted)),
        out_specs=(vm, vm),
        scratch_shapes=[
            pltpu.VMEM((2, 2, H, W + 128), jnp.bfloat16),
            pltpu.VMEM((W // 128, H, 128), jnp.float32),
            pltpu.SMEM((8, 128), jnp.int32),
            pltpu.SemaphoreType.DMA,
        ],
        compiler_params=pltpu.CompilerParams(vmem_limit_bytes=16 << 20),
        name="render",
    )(first, count, *fitted)


def per_device(points, source, slab_first, slab_count):
    points, source = [pltpu.with_memory_space_constraint(x, pltpu.HBM) for x in (points, source)]
    return render(slab_first, slab_count, fit(points, source))


def solution(mesh):
    return jax.shard_map(
        per_device,
        mesh=mesh,
        in_specs=(
            P(None, ("sec", "ty")),
            P(("sec", "ty"), None),
            P(("sec", "ty")),
            P(("sec", "ty")),
        ),
        out_specs=(P(("sec", "ty"), None), P(None, ("sec", "ty"), None)),
        check_vma=False,
    )
```
